256 devices in a mesh: row: 16 (over y, x), col: 16 (over z, core).
Axes of the slice: x: 4, y: 4, z: 8, core: 2. Of those that a mesh axis runs over, the one named last changes fastest.
Arguments:
- tile_data: bfloat16 [1024, 128, 128], P(('row', 'col')), may hold values from -24 to 24
- tile_coords: int32 [3, 1024], P(None, ('row', 'col')), may hold values from 0 to 2047, as said below
- tile_counts: int32 [256], P(('row', 'col')), may hold values from 1 to 4, as said below
- factor_rows: float32 [64, 32768], P(None, ('row', 'col')), may hold values from -6 to 6
- factor_cols: float32 [64, 32768], P(None, ('col', 'row')), may hold values from -6 to 6
- factor_depth: float32 [64, 2048], P(None, ('row', 'col')), may hold values from -6 to 6
- damping: float32 [], replicated, may hold values from 128 to 512
Outputs:
- step_a: float32 [64, 32768], P(None, ('row', 'col'))
- step_b: float32 [64, 32768], P(None, ('col', 'row'))
- step_c: float32 [64, 2048], P(None, ('row', 'col'))
The draws below stay inside these ranges and needn't reach their ends.
Inputs may be any that keep to these rules, and one draw needn't show every extreme that they name: `tile_coords`: the first row names a tile's block within its device's group of 16 first-mode blocks, the second its block within the group of 16 second-mode blocks, the third its third-mode index below 2048. `tile_counts`: slots at and beyond a device's count are padding and carry nothing; some device fills all 4 slots.
All inputs are finite; a program needn't handle non-finite values.
Results may differ from the reference program's by a relative error of at most 0.0003.
Values sent between devices are 32-bit elements; how exact they have to be, the bound alone decides.
A program may use at most 64 MiB of HBM per device.

```python
import math
import jax
import jax.numpy as jnp
from jax import lax

RANK = 64
TILE = 128
RB = 16
CB = 16
TCAP = 4
ITERS = 2
MODE_ROWS = 32768
MODE_COLS = 32768
DEPTH = 2048
TILES_ALL = 1024
N_ROW = 16
N_COL = 16


def draw_tile_coords(key, part):
    key_rows, key_cols, key_depth = jax.random.split(key, 3)
    block_rows = jax.random.randint(key_rows, (TILES_ALL,), 0, RB)
    block_cols = jax.random.randint(key_cols, (TILES_ALL,), 0, CB)
    depth_index = jax.random.randint(key_depth, (TILES_ALL,), 0, DEPTH)
    return jnp.stack([block_rows, block_cols, depth_index]).astype(jnp.int32)


def draw_tile_counts(key, part):
    key_base, key_top = jax.random.split(key, 2)
    device_total = N_ROW * N_COL
    base_counts = jax.random.randint(key_base, (device_total,), TCAP // 4, TCAP + 1)
    fullest = jax.random.randint(key_top, (), 0, device_total)
    placed = jnp.arange(device_total, dtype=jnp.int32) == fullest
    return jnp.where(placed, TCAP, base_counts).astype(jnp.int32)


def level_of(stream_key, shape, cuts, least, largest):
    loudness, own = 1.0, jax.random.fold_in(stream_key, 6)
    for position, shards_of in cuts:
        heights = jnp.exp(jax.random.uniform(jax.random.fold_in(own, position), (shards_of,), jnp.float32, least / len(cuts), largest / len(cuts)))
        loudness = loudness * jnp.repeat(heights, shape[position] // shards_of).reshape([-1 if axis == position else 1 for axis in range(len(shape))])
    return loudness


def noise(stream_key, shape, spread, most, cuts=(), kind=jnp.bfloat16):
    factor_of = level_of(stream_key, shape, cuts, -0.22, 0.18) if cuts else 1.0
    result = jax.random.normal(stream_key, shape, jnp.float32) * spread * factor_of
    return jnp.minimum(jnp.maximum(result, -most), most).astype(kind)


def setup_inputs(seed: int = 0) -> dict:
    arg_keys = jax.random.split(jax.random.key(seed), 8)
    tile_data = noise(arg_keys[0], (TILES_ALL, TILE, TILE), 4.0, 24.0, ((0, 256),))
    tile_coords = draw_tile_coords(jax.random.fold_in(arg_keys[7], 71), 0)
    tile_counts = draw_tile_counts(jax.random.fold_in(arg_keys[7], 71), 0)
    factor_rows = noise(arg_keys[3], (RANK, MODE_ROWS), 1.0, 6.0, ((1, 256),), jnp.float32)
    factor_cols = noise(arg_keys[4], (RANK, MODE_COLS), 1.0, 6.0, ((1, 256),), jnp.float32)
    factor_depth = noise(arg_keys[5], (RANK, DEPTH), 1.0, 6.0, ((1, 256),), jnp.float32)
    damping = jnp.clip(jnp.exp(jax.random.uniform(arg_keys[6], (), jnp.float32, math.log(128.0), math.log(512.0))), 128.0, 512.0)
    return {"tile_data": tile_data, "tile_coords": tile_coords, "tile_counts": tile_counts, "factor_rows": factor_rows, "factor_cols": factor_cols, "factor_depth": factor_depth, "damping": damping}


exact_precision = lax.Precision.HIGHEST


def make_onehot(indices, block_count):
    return (indices[:, None] == jnp.arange(block_count, dtype=jnp.int32)[None, :]).astype(jnp.float32)


def pick_rows(onehot, blocks):
    shaped = blocks.reshape(blocks.shape[0], onehot.shape[1], blocks.shape[1] // onehot.shape[1])
    return jnp.einsum('tq,rqa->tra', onehot.astype(blocks.dtype), shaped, precision=exact_precision)


def fold_rows(onehot, grads):
    summed = jnp.einsum('tq,tra->rqa', onehot.astype(grads.dtype), grads, precision=exact_precision)
    return summed.reshape(summed.shape[0], summed.shape[1] * summed.shape[2])


def tile_model(rows_a, rows_b, rows_c):
    return jnp.einsum('tra,trb->tab', rows_a, rows_b * rows_c[:, :, None], precision=exact_precision)


def tile_products(rows_a, rows_b, rows_c, dir_a, dir_b, dir_c):
    depth_cols = rows_c[:, :, None]
    left_side = jnp.concatenate([dir_a, rows_a, rows_a], axis=1)
    right_side = jnp.concatenate([rows_b * depth_cols, dir_b * depth_cols, rows_b * dir_c[:, :, None]], axis=1)
    return jnp.einsum('tra,trb->tab', left_side, right_side, precision=exact_precision)


def tile_transpose(values, rows_a, rows_b, rows_c):
    depth_cols = rows_c[:, :, None]
    row_raw = jnp.einsum('tab,trb->tra', values, rows_b, precision=exact_precision)
    grad_rows = row_raw * depth_cols
    grad_cols = jnp.einsum('tab,tra->trb', values, rows_a * depth_cols, precision=exact_precision)
    grad_depth = jnp.sum(rows_a * row_raw, axis=2)
    return grad_rows, grad_cols, grad_depth


def reference(tile_data, tile_coords, tile_counts, factor_rows, factor_cols, factor_depth, damping):
    rows_group = RB * TILE
    cols_group = CB * TILE

    def apply_all(direction):
        def per_device(device, totals):
            device = jnp.asarray(device).astype(jnp.int32)
            grid_row = device // N_COL
            grid_col = device % N_COL
            start_a = (grid_row * rows_group).astype(jnp.int32)
            start_b = (grid_col * cols_group).astype(jnp.int32)
            block_a = lax.dynamic_slice_in_dim(factor_rows, start_a, rows_group, 1)
            block_b = lax.dynamic_slice_in_dim(factor_cols, start_b, cols_group, 1)
            coords_here = lax.dynamic_slice_in_dim(tile_coords, (device * TCAP).astype(jnp.int32), TCAP, 1)
            live_mask = (jnp.arange(TCAP, dtype=jnp.int32) < tile_counts[device]).astype(factor_rows.dtype)[:, None, None]
            pick_a = make_onehot(coords_here[0], RB)
            pick_b = make_onehot(coords_here[1], CB)
            rows_a = pick_rows(pick_a, block_a)
            rows_b = pick_rows(pick_b, block_b)
            rows_c = jnp.take(factor_depth, coords_here[2], axis=1).T
            if direction is None:
                data_here = lax.dynamic_slice_in_dim(tile_data, (device * TCAP).astype(jnp.int32), TCAP, 0).astype(factor_rows.dtype)
                values = data_here - tile_model(rows_a, rows_b, rows_c)
            else:
                dir_block_a = lax.dynamic_slice_in_dim(direction[0], start_a, rows_group, 1)
                dir_block_b = lax.dynamic_slice_in_dim(direction[1], start_b, cols_group, 1)
                dir_c = jnp.take(direction[2], coords_here[2], axis=1).T
                values = tile_products(rows_a, rows_b, rows_c, pick_rows(pick_a, dir_block_a), pick_rows(pick_b, dir_block_b), dir_c)
            grad_rows, grad_cols, grad_depth = tile_transpose(values * live_mask, rows_a, rows_b, rows_c)
            old_a = lax.dynamic_slice_in_dim(totals[0], start_a, rows_group, 1)
            total_a = lax.dynamic_update_slice_in_dim(totals[0], old_a + fold_rows(pick_a, grad_rows), start_a, 1)
            old_b = lax.dynamic_slice_in_dim(totals[1], start_b, cols_group, 1)
            total_b = lax.dynamic_update_slice_in_dim(totals[1], old_b + fold_rows(pick_b, grad_cols), start_b, 1)
            total_c = totals[2] + jax.ops.segment_sum(grad_depth, coords_here[2], num_segments=DEPTH).T
            return (total_a, total_b, total_c)

        start = (jnp.zeros_like(factor_rows), jnp.zeros_like(factor_cols), jnp.zeros_like(factor_depth))
        return lax.fori_loop(0, N_ROW * N_COL, per_device, start)

    def hessian(direction):
        applied = apply_all(direction)
        return tuple(part_one + damping * part_two for part_one, part_two in zip(applied, direction))

    def inner(first, second):
        return sum(jnp.sum(part_one * part_two) for part_one, part_two in zip(first, second))

    rhs = apply_all(None)
    solution = tuple(jnp.zeros_like(member) for member in rhs)
    residual = rhs
    direction = rhs
    norm_now = inner(residual, residual)
    for iteration in range(ITERS):
        image_vec = hessian(direction)
        step_size = norm_now / inner(direction, image_vec)
        solution = tuple(sol + step_size * dvec for sol, dvec in zip(solution, direction))
        residual = tuple(res - step_size * ivec for res, ivec in zip(residual, image_vec))
        norm_next = inner(residual, residual)
        direction = tuple(res + (norm_next / norm_now) * dvec for res, dvec in zip(residual, direction))
        norm_now = norm_next
    return (solution[0], solution[1], solution[2])
```

```python
import jax
import jax.numpy as jnp
from jax import lax
from jax.experimental import pallas as pl
from jax.experimental.pallas import tpu as pltpu
from jax.sharding import PartitionSpec as P

G = 16
T = 4
RS = 4
F32 = jnp.float32
EXACT = lax.Precision.HIGHEST

COL_PEERS = [(dz, dc) for dz in (4, 3, 5, 2, 6, 1, 7) for dc in (0, 1)] + [(0, 1)]
ROW_PEERS = sorted(
    [(dy, dx) for dy in range(4) for dx in range(4) if (dy, dx) != (0, 0)],
    key=lambda d: -(min(d[0], 4 - d[0]) + min(d[1], 4 - d[1])),
)


def dot(a, b, dims):
    return lax.dot_general(a, b, (dims, ((), ())), precision=EXACT, preferred_element_type=F32)


def iota(shape, dim):
    return lax.broadcasted_iota(jnp.int32, shape, dim)


def kernel(
    coords, counts, damp, fa, fb, fc, data_hbm,
    out_a, out_b, out_c,
    data, cs0, cr0, rs0, rr0, cs1, cr1, rs1, rr1,
    cs2, cr2, rs2, rr2, cs3, cr3, rs3, rr3,
    cs4, cr4, rs4, rr4, cs5, cr5, rs5, rr5,
    cs6, cr6, rs6, rr6, cso, cro, rso, rro,
    va, vb, ga, gb, ta, tb, tat, da, db, jg, wa, wat, wb, wbt,
    data_sem, send_sem, recv_sem,
):
    p = lax.axis_index("row")
    q = lax.axis_index("col")
    col_of = []
    z, core = q // 2, q % 2
    for dz, dc in COL_PEERS:
        col_of.append(((z + dz) % 8) * 2 + (core + dc) % 2)
    row_of = []
    y, x = p // 4, p % 4
    for dy, dx in ROW_PEERS:
        row_of.append(((y + dy) % 4) * 4 + (x + dx) % 4)

    load = pltpu.make_async_copy(data_hbm, data, data_sem)
    load.start()

    barrier = pltpu.get_barrier_semaphore()
    for peer in col_of:
        pl.semaphore_signal(barrier, inc=1, device_id={"col": peer})
    for peer in row_of:
        pl.semaphore_signal(barrier, inc=1, device_id={"row": peer})

    def send(hop, axis, src, dst):
        me, peers, name = (q, col_of, "col") if axis == 0 else (p, row_of, "row")
        for peer in peers:
            pltpu.make_async_remote_copy(
                src_ref=src.at[peer],
                dst_ref=dst.at[me],
                send_sem=send_sem.at[hop, axis],
                recv_sem=recv_sem.at[hop, axis],
                device_id={name: peer},
            ).start()
        dst[me] = src[me]

    def wait(sem, ref):
        some = ref.at[pl.ds(0, G - 1)]
        pltpu.make_async_copy(some, some, sem).wait()

    def arrived(hop, axis, dst):
        wait(recv_sem.at[hop, axis], dst)

    lane = iota((1, 128), 1)

    def positions(coord_row, member):
        base = (member % 8) * 16
        here = lane - base
        val = jnp.zeros((1, 128), F32)
        for t in range(T):
            at = (here // RS == t) & (here >= 0)
            val = jnp.where(at, (coords[coord_row, t] * RS + here % RS).astype(F32), val)
        first = member // 8 == 0
        zero = jnp.zeros((1, 128), F32)
        return jnp.where(first, val, zero), jnp.where(first, zero, val)

    def depth_index(member):
        here = lane - member * 8
        val = jnp.zeros((1, 128), F32)
        for t in range(T):
            at = (here >= 0) & (here < 8) & (here % T == t)
            val = jnp.where(at, coords[2, t].astype(F32), val)
        return val

    zero_row = jnp.zeros((1, 128), F32)
    low, high = positions(0, q)
    info_col = jnp.concatenate([low, high, depth_index(q), zero_row], axis=0)
    low, high = positions(1, p)
    info_row = jnp.concatenate([low, high, depth_index(p), zero_row], axis=0)
    own = jnp.concatenate([jnp.zeros((64, 128), F32), jnp.pad(fc[...], ((0, 0), (0, 120)))], axis=0)
    own = jnp.transpose(own)[:8]
    for j in range(G):
        cs0[j, 0:4] = fa[4 * j:4 * j + 4]
        cs0[j, 4:8] = info_col
        cs0[j, 8:16] = own
        rs0[j, 0:4] = fb[4 * j:4 * j + 4]
        rs0[j, 4:8] = info_row

    pl.semaphore_wait(barrier, 2 * (G - 1))
    send(0, 0, cs0, cr0)
    send(0, 1, rs0, rr0)
    arrived(0, 0, cr0)
    arrived(0, 1, rr0)

    info_col = jnp.sum(cr0[:, 0:8], axis=0)
    info_row = jnp.sum(rr0[:, 0:8], axis=0)

    def matrices(info, w, wt):
        turned = jnp.transpose(info)
        for half in range(2):
            across = info[4 + half:5 + half].astype(jnp.int32)
            down = turned[:, 4 + half:5 + half].astype(jnp.int32)
            w[:, 128 * half:128 * half + 128] = (iota((64, 128), 0) == across).astype(F32)
            wt[128 * half:128 * half + 128] = (iota((128, 64), 1) == down).astype(F32)
        return turned

    matrices(info_col, wa, wat)
    turned = matrices(info_row, wb, wbt)
    k_here = info_col[6:7].astype(jnp.int32)
    k_there = turned[:, 6:7].astype(jnp.int32)
    down, across = iota((128, 128), 0), iota((128, 128), 1)
    slot_row = down % 8 < T
    own_index = (down // 8) * 128 + q * 8 + down % 8
    mix0 = (slot_row & (k_there == across + p * 128)).astype(F32)
    target = jnp.where(across % 8 < T, own_index, k_there)
    allowed = jnp.where(across % 8 < T, 1.0, slot_row.astype(F32))
    mix = (jnp.broadcast_to(k_here, (128, 128)) == target).astype(F32) * allowed

    def serve(wt, v, dst):
        s = dot(wt[...], v[...], ((1,), (0,)))
        dst[:, 0:16] = s.reshape(G, 16, 128)

    def mixed(m, tiles, dst):
        u = dot(m, tiles.reshape(128, 128), ((1,), (0,)))
        dst[:, 16:24] = u.reshape(G, 8, 128)

    for j in range(G):
        va[4 * j:4 * j + 4] = cr0[j, 0:4]
        vb[4 * j:4 * j + 4] = rr0[j, 0:4]
    serve(wat, va, cs1)
    send(1, 0, cs1, cr1)
    mixed(mix0, cr0[:, 8:16], rs1)
    serve(wbt, vb, rs1)
    send(1, 1, rs1, rr1)

    def unpack(src, dst):
        for t in range(T):
            for j in range(G):
                dst[t, 4 * j:4 * j + 4] = src[j, 4 * t:4 * t + 4]

    def pack(t, value, dst):
        for j in range(G):
            dst[j, 4 * t:4 * t + 4] = value[4 * j:4 * j + 4]

    def depth_of(src):
        total = jnp.sum(src[:, 16:24], axis=0)
        return total, jnp.transpose(total)

    arrived(1, 0, cr1)
    unpack(cr1, ta)
    arrived(1, 1, rr1)
    unpack(rr1, tb)
    total, turned_c = depth_of(rr1)
    depth = [jnp.broadcast_to(turned_c[64:128, t:t + 1], (64, 128)) for t in range(T)]
    load.wait()

    def gradients(t, values, cs, rs, cols):
        raw = dot(tb[t], values, ((1,), (1,)))
        pack(t, raw * depth[t], cs)
        pack(t, dot(ta[t] * depth[t], values, ((1,), (0,))), rs)
        col = jnp.sum(ta[t] * raw, axis=1, keepdims=True)
        lanes = iota((64, 128), 1)
        left = cols[0] + jnp.where(lanes == t, col, 0.0)
        right = cols[1] + jnp.where(lanes == t + T, col, 0.0)
        return left, right

    def depth_message(cols, cs):
        tile = jnp.transpose(jnp.concatenate(cols, axis=0))[:8]
        for j in range(G):
            cs[j, 16:24] = tile

    def live(t):
        return (t < counts[0]).astype(F32)

    cols = (jnp.zeros((64, 128), F32), jnp.zeros((64, 128), F32))
    for t in range(T):
        tat[t] = jnp.transpose(ta[t])
        model = dot(tat[t], tb[t] * depth[t], ((1,), (0,)))
        values = (data[t].astype(F32) - model) * live(t)
        cols = gradients(t, values, cs2, rs2, cols)
    depth_message(cols, cs2)
    send(2, 0, cs2, cr2)
    send(2, 1, rs2, rr2)

    def fold(w, src, v):
        v[...] = dot(w[...], src.reshape(256, 128), ((1,), (0,)))

    half_mask = ((down % 8 < T) == (across < 64)).astype(F32)

    def masked(src):
        return src[:, 16:24].reshape(128, 128) * half_mask

    arrived(2, 0, cr2)
    fold(wa, cr2[:, 0:16], ga)
    serve(wat, ga, cs3)
    send(3, 0, cs3, cr3)
    arrived(2, 1, rr2)
    fold(wb, rr2[...], gb)
    serve(wbt, gb, rs3)
    mixed(mix, masked(cr2), rs3)
    send(3, 1, rs3, rr3)
    arrived(3, 0, cr3)
    unpack(cr3, da)
    arrived(3, 1, rr3)
    unpack(rr3, db)
    total_g, turned_g = depth_of(rr3)

    def jacobian(t, turned_u):
        du = jnp.broadcast_to(turned_u[64:128, t:t + 1], (64, 128))
        right = db[t] * depth[t] + tb[t] * du
        left = jnp.transpose(da[t])
        return dot(left, tb[t] * depth[t], ((1,), (0,))) + dot(tat[t], right, ((1,), (0,)))

    def norm(value):
        return jnp.sum(value, axis=(0, 1), keepdims=True)

    cols = (jnp.zeros((64, 128), F32), jnp.zeros((64, 128), F32))
    squares = jnp.zeros((128, 128), F32)
    for t in range(T):
        values = jacobian(t, turned_g) * live(t)
        jg[t] = values
        squares = squares + values * values
        cols = gradients(t, values, cs4, rs4, cols)
    own_g = total_g[:, 0:64]
    g_part = norm(ga[...] * ga[...]) + norm(gb[...] * gb[...]) + norm(own_g * own_g)
    j_part = norm(squares)
    tile = jnp.transpose(jnp.concatenate(cols, axis=0))[:8]
    row8, lane8 = iota((8, 128), 0), iota((8, 128), 1)
    tile = jnp.where((row8 == 0) & (lane8 >= 64), g_part, tile)
    tile = jnp.where((row8 == 1) & (lane8 >= 64), j_part, tile)
    for j in range(G):
        cs4[j, 16:24] = tile
    send(4, 0, cs4, cr4)
    send(4, 1, rs4, rr4)

    arrived(4, 0, cr4)
    fold(wa, cr4[:, 0:16], va)
    serve(wat, va, cs5)
    send(5, 0, cs5, cr5)
    group = jnp.sum(cr4[:, 16:24], axis=0)
    arrived(4, 1, rr4)
    fold(wb, rr4[...], vb)
    serve(wbt, vb, rs5)
    u = dot(mix, masked(cr4), ((1,), (0,)))
    up = (across >= 64) & (down % 8 >= T)
    u = jnp.where(up & (down % 8 == 4), jnp.broadcast_to(group[0:1, 127:128], (128, 128)), u)
    u = jnp.where(up & (down % 8 == 5), jnp.broadcast_to(group[1:2, 127:128], (128, 128)), u)
    rs5[:, 16:24] = u.reshape(G, 8, 128)
    send(5, 1, rs5, rr5)

    for j in range(G):
        cso[j, 0:4] = ga[4 * j:4 * j + 4]
        cso[j, 4:8] = va[4 * j:4 * j + 4]
        rso[j, 0:4] = gb[4 * j:4 * j + 4]
        rso[j, 4:8] = vb[4 * j:4 * j + 4]
    send(6, 0, cso, cro)
    send(6, 1, rso, rro)

    arrived(5, 0, cr5)
    unpack(cr5, da)
    arrived(5, 1, rr5)
    unpack(rr5, db)
    total_w, turned_w = depth_of(rr5)
    lam = damp[0]
    g_norm = total_w[4:5, 127:128]
    j_norm = total_w[5:6, 127:128]
    alpha0 = g_norm / (j_norm + lam * g_norm)

    def residual_of(g, w):
        return g - alpha0 * (w + lam * g)

    own_w = total_w[:, 0:64]
    r_a = residual_of(ga[...], va[...])
    r_b = residual_of(gb[...], vb[...])
    r_c = residual_of(own_g, own_w)
    rr_part = norm(r_a * r_a) + norm(r_b * r_b) + norm(r_c * r_c)
    rg_part = norm(r_a * ga[...]) + norm(r_b * gb[...]) + norm(r_c * own_g)
    square = jnp.zeros((128, 128), F32)
    cross = jnp.zeros((128, 128), F32)
    for t in range(T):
        jw = jacobian(t, turned_w) * live(t)
        jr = residual_of(jg[t], jw)
        square = square + jr * jr
        cross = cross + jr * jg[t]

    parts = (rr_part, rg_part, norm(square), norm(cross))
    tile = jnp.zeros((8, 128), F32)
    for i, part in enumerate(parts):
        tile = jnp.where(row8 == i, part, tile)
    for j in range(G):
        cs6[j] = tile
    send(7, 0, cs6, cr6)
    arrived(7, 0, cr6)
    tile = jnp.sum(cr6[...], axis=0)
    for j in range(G):
        rs6[j] = tile
    send(7, 1, rs6, rr6)

    arrived(6, 0, cro)
    arrived(6, 1, rro)
    arrived(7, 1, rr6)
    tile = jnp.sum(rr6[...], axis=0)
    r_norm, r_g, jr_norm, jr_jg = [tile[i:i + 1, 0:1] for i in range(4)]
    beta = r_norm / g_norm
    curve = (
        jr_norm + lam * r_norm
        + 2.0 * beta * (jr_jg + lam * r_g)
        + beta * beta * (j_norm + lam * g_norm)
    )
    alpha1 = r_norm / curve

    def step(g, w):
        return alpha0 * g + alpha1 * (residual_of(g, w) + beta * g)

    for j in range(G):
        out_a[4 * j:4 * j + 4] = step(cro[j, 0:4], cro[j, 4:8])
        out_b[4 * j:4 * j + 4] = step(rro[j, 0:4], rro[j, 4:8])
    out_c[...] = step(turned_g[0:64, 0:8], turned_w[0:64, 0:8])

    for hop, axis, src in (
        (0, 0, cs0), (0, 1, rs0), (1, 0, cs1), (1, 1, rs1), (2, 0, cs2), (2, 1, rs2),
        (3, 0, cs3), (3, 1, rs3), (4, 0, cs4), (4, 1, rs4), (5, 0, cs5), (5, 1, rs5),
        (6, 0, cso), (6, 1, rso), (7, 0, cs6), (7, 1, rs6),
    ):
        wait(send_sem.at[hop, axis], src)


def per_device(
    tile_data, tile_coords, tile_counts, factor_rows, factor_cols, factor_depth, damping
):
    vmem = pl.BlockSpec(memory_space=pltpu.VMEM)
    smem = pl.BlockSpec(memory_space=pltpu.SMEM)
    rows = lambda n: pltpu.VMEM((G, n, 128), F32)
    pair = lambda n: [rows(n), rows(n)]
    return pl.pallas_call(
        kernel,
        out_shape=(
            jax.ShapeDtypeStruct((64, 128), F32),
            jax.ShapeDtypeStruct((64, 128), F32),
            jax.ShapeDtypeStruct((64, 8), F32),
        ),
        in_specs=[smem, smem, smem, vmem, vmem, vmem, pl.BlockSpec(memory_space=pl.ANY)],
        out_specs=(vmem, vmem, vmem),
        scratch_shapes=[
            pltpu.VMEM((T, 128, 128), jnp.bfloat16),
            *pair(16), *pair(8),
            *pair(16), *pair(24),
            *pair(24), *pair(16),
            *pair(16), *pair(24),
            *pair(24), *pair(16),
            *pair(16), *pair(24),
            *pair(8), *pair(8),
            *pair(8), *pair(8),
            *[pltpu.VMEM((64, 128), F32)] * 4,
            *[pltpu.VMEM((T, 64, 128), F32)] * 2,
            pltpu.VMEM((T, 128, 64), F32),
            *[pltpu.VMEM((T, 64, 128), F32)] * 2,
            pltpu.VMEM((T, 128, 128), F32),
            pltpu.VMEM((64, 256), F32), pltpu.VMEM((256, 64), F32),
            pltpu.VMEM((64, 256), F32), pltpu.VMEM((256, 64), F32),
            pltpu.SemaphoreType.DMA,
            pltpu.SemaphoreType.DMA((8, 2)),
            pltpu.SemaphoreType.DMA((8, 2)),
        ],
        compiler_params=pltpu.CompilerParams(collective_id=0, has_side_effects=True),
        name="gauss_newton",
    )(
        tile_coords, tile_counts, damping.reshape(1),
        factor_rows, factor_cols, factor_depth, tile_data,
    )


def solution(mesh):
    both = ("row", "col")
    flip = ("col", "row")
    return jax.shard_map(
        per_device,
        mesh=mesh,
        in_specs=(
            P(both, None, None), P(None, both), P(both),
            P(None, both), P(None, flip), P(None, both), P(),
        ),
        out_specs=(P(None, both), P(None, flip), P(None, both)),
        check_vma=False,
    )
```

```python
import jax
import jax.numpy as jnp
from jax import lax
from jax.experimental import pallas as pl
from jax.experimental.pallas import tpu as pltpu
from jax.sharding import PartitionSpec as P

G = 16
T = 4
RS = 4
F32 = jnp.float32
BF16 = jnp.bfloat16

COL_PEERS = [(dz, dc) for dz in (4, 3, 5, 2, 6, 1, 7) for dc in (0, 1)] + [(0, 1)]
ROW_PEERS = sorted(
    [(dy, dx) for dy in range(4) for dx in range(4) if (dy, dx) != (0, 0)],
    key=lambda d: -(min(d[0], 4 - d[0]) + min(d[1], 4 - d[1])),
)

EXCHANGES = (
    ("a_slices", 0, 8), ("a_depth", 0, 4), ("b_slices", 1, 8),
    ("a_slots", 0, 16), ("b_slots", 1, 16), ("c_slots", 1, 8),
    ("ga_in", 0, 16), ("gc_in", 0, 4), ("gb_in", 1, 16),
    ("ga_out", 0, 16), ("gb_out", 1, 16), ("gc_out", 1, 8),
    ("wa_in", 0, 16), ("wc_in", 0, 4), ("wb_in", 1, 16),
    ("wa_out", 0, 16), ("wb_out", 1, 16), ("wc_out", 1, 8),
    ("a_put", 0, 8), ("b_put", 1, 8),
    ("sum_col", 0, 1), ("sum_row", 1, 1),
)
INDEX = {name: i for i, (name, _, _) in enumerate(EXCHANGES)}


def mm(a, b, rhs_dim=0):
    return lax.dot_general(a, b, (((1,), (rhs_dim,)), ((), ())), preferred_element_type=F32)


def two(x):
    high = x.astype(BF16)
    return high, (x - high.astype(F32)).astype(BF16)


def three(x, axis=0):
    high = x.astype(BF16)
    rest = x - high.astype(F32)
    mid = rest.astype(BF16)
    low = (rest - mid.astype(F32)).astype(BF16)
    return jnp.concatenate([high, mid, low], axis=axis)


def mm_two(left, right, rhs_dim=0):
    rows = left.shape[0] // 2
    high, low = right
    both = mm(left, high, rhs_dim)
    return both[:rows] + both[rows:] + mm(left[:rows], low, rhs_dim)


def iota(shape, dim):
    return lax.broadcasted_iota(jnp.int32, shape, dim)


def kernel(coords_hbm, counts_hbm, damp_hbm, fa_hbm, fb_hbm, fc_hbm, data_hbm, *refs):
    out_a, out_b, out_c = refs[:3]
    refs = refs[3:]
    n = len(EXCHANGES)
    outbox, inbox = refs[:n], refs[n:2 * n]
    (
        coords, counts, damp, fa, fb, fc, data,
        va, vb, ga, gb, ta, tb, da, db, jg,
        at2, tb2, tac2, bc_high, bc_low, left, xc,
        wa, wb, wat, wbt, mix, load_sem, send_sem, recv_sem,
    ) = refs[2 * n:]
    p = lax.axis_index("row")
    q = lax.axis_index("col")
    z, core = q // 2, q % 2
    col_of = [((z + dz) % 8) * 2 + (core + dc) % 2 for dz, dc in COL_PEERS]
    y, x = p // 4, p % 4
    row_of = [((y + dy) % 4) * 4 + (x + dx) % 4 for dy, dx in ROW_PEERS]

    barrier = pltpu.get_barrier_semaphore()
    for peer in col_of:
        pl.semaphore_signal(barrier, inc=1, device_id={"col": peer})
    for peer in row_of:
        pl.semaphore_signal(barrier, inc=1, device_id={"row": peer})

    loads = [
        pltpu.make_async_copy(src, dst, load_sem.at[i])
        for i, (src, dst) in enumerate((
            (coords_hbm, coords), (counts_hbm, counts), (damp_hbm, damp),
            (fa_hbm, fa), (fb_hbm, fb), (fc_hbm, fc), (data_hbm, data),
        ))
    ]
    for load in loads:
        load.start()

    def box(name):
        return outbox[INDEX[name]], inbox[INDEX[name]]

    def send(name):
        i = INDEX[name]
        me, peers, axis = ((q, col_of, "col"), (p, row_of, "row"))[EXCHANGES[i][1]]
        src, dst = outbox[i], inbox[i]
        for peer in peers:
            pltpu.make_async_remote_copy(
                src_ref=src.at[peer],
                dst_ref=dst.at[me],
                send_sem=send_sem.at[i],
                recv_sem=recv_sem.at[i],
                device_id={axis: peer},
            ).start()
        dst[me] = src[me]

    def wait(sem, ref):
        some = ref.at[pl.ds(0, G - 1)]
        pltpu.make_async_copy(some, some, sem).wait()

    def arrived(name):
        i = INDEX[name]
        wait(recv_sem.at[i], inbox[i])
        return inbox[i]

    lane = iota((1, 128), 1)
    zero_row = jnp.zeros((1, 128), F32)

    def positions(coord_row, member):
        here = lane - (member % 8) * 16
        val = zero_row
        for t in range(T):
            at = (here >= RS * t) & (here < RS * t + RS)
            val = jnp.where(at, (coords[coord_row, t] * RS + here - RS * t).astype(F32), val)
        first = member // 8 == 0
        return jnp.where(first, val, zero_row), jnp.where(first, zero_row, val)

    def depth_index(member):
        here = lane - member * 8
        val = zero_row
        for t in range(T):
            at = (here == t) | (here == t + T)
            val = jnp.where(at, coords[2, t].astype(F32), val)
        return val

    loads[0].wait()
    first, second = positions(0, q)
    info_col = jnp.concatenate([first, second, depth_index(q), zero_row], axis=0)
    first, second = positions(1, p)
    info_row = jnp.concatenate([first, second, depth_index(p), zero_row], axis=0)
    for load in loads[3:6]:
        load.wait()
    own = jnp.concatenate([fc[0:4], fc[4:8]], axis=1)
    a_slices, a_depth, b_slices = box("a_slices")[0], box("a_depth")[0], box("b_slices")[0]
    for j in range(G):
        a_slices[j, 0:4] = fa[4 * j:4 * j + 4]
        a_slices[j, 4:8] = info_col
        a_depth[j] = own
        b_slices[j, 0:4] = fb[4 * j:4 * j + 4]
        b_slices[j, 4:8] = info_row

    pl.semaphore_wait(barrier, 2 * (G - 1))
    send("a_slices")
    send("b_slices")
    send("a_depth")

    def across_of(info):
        return jnp.concatenate([info[4:5], info[5:6]], axis=1).astype(jnp.int32)

    def back_matrix(info, dst):
        turned = jnp.transpose(info).astype(jnp.int32)
        lanes = iota((128, 64), 1)
        for half in range(2):
            w = (lanes == turned[:, 4 + half:5 + half]).astype(BF16)
            dst[128 * half:128 * half + 128] = jnp.concatenate([w, w, w], axis=1)
        return turned

    def serve(w, v, name):
        s = mm(w[...], three(v))
        box(name)[0][...] = s.reshape(G, 16, 128)
        send(name)

    def stacked(src):
        for j in range(G):
            xc[4 * j:4 * j + 4] = src[j]
        return xc[...]

    src = arrived("b_slices")
    info_row = jnp.sum(src[...], axis=0)
    turned = back_matrix(info_row, wbt)
    for j in range(G):
        vb[4 * j:4 * j + 4] = src[j, 0:4]
    serve(wbt, vb[...], "b_slots")
    src = arrived("a_slices")
    info_col = jnp.sum(src[...], axis=0)
    back_matrix(info_col, wat)
    for j in range(G):
        va[4 * j:4 * j + 4] = src[j, 0:4]
    serve(wat, va[...], "a_slots")
    src = arrived("a_depth")
    k_there = turned[:, 6:7]
    down, half = iota((128, 64), 0), iota((128, 64), 1)
    column = p * 128 + (half // 4) * 8 + half % 4
    slot_row = (down % 8 < T).astype(F32)
    pick = [
        ((k_there == column + 4 * i).astype(F32) * slot_row).astype(BF16) for i in range(2)
    ]
    pick = jnp.concatenate(pick, axis=0)
    both = mm(jnp.concatenate([pick, pick, pick], axis=1), three(stacked(src)))
    c_out = box("c_slots")[0]
    c_out[...] = (pltpu.roll(both[:128], 64, 1) + both[128:]).reshape(G, 8, 128)
    send("c_slots")

    wa[...] = (iota((64, 256), 0) == across_of(info_col)).astype(BF16)
    wb[...] = (iota((64, 256), 0) == across_of(info_row)).astype(BF16)

    spread = (iota((128, 64), 0) == (half // 4) * 8 + half % 4).astype(BF16)
    k_tiles = jnp.broadcast_to(info_col[6:7], (8, 128))
    k_lane = mm(three(k_tiles, 1), jnp.concatenate([spread, spread, spread], axis=0))
    k_lane = k_lane[0:1].astype(jnp.int32)
    own_index = (down // 8) * 128 + q * 8 + down % 8
    to_own = (k_lane == own_index).astype(BF16)
    to_slot = ((k_lane == k_there).astype(F32) * slot_row).astype(BF16)
    to_both = jnp.concatenate([to_own, to_slot], axis=0)
    mix[...] = jnp.concatenate([to_both, to_both, to_both], axis=1)

    def unpack(src, dst):
        for t in range(T):
            for j in range(G):
                dst[t, 4 * j:4 * j + 4] = src[j, 4 * t:4 * t + 4]

    def pack(t, value, dst):
        for j in range(G):
            dst[j, 4 * t:4 * t + 4] = value[4 * j:4 * j + 4]

    def columns(turned):
        return [jnp.broadcast_to(turned[64:128, t:t + 1], (64, 128)) for t in range(T)]

    src = arrived("b_slots")
    unpack(src, tb)
    for t in range(T):
        high, low = two(tb[t])
        tb2[t, 0:64] = high
        tb2[t, 64:128] = low
    src = arrived("c_slots")
    depth = columns(jnp.transpose(jnp.sum(src[...], axis=0)))
    for t in range(T):
        bc_high[t], bc_low[t] = two(tb[t] * depth[t])
    for load in (loads[1], loads[2], loads[6]):
        load.wait()
    src = arrived("a_slots")
    unpack(src, ta)

    def live(t):
        return (t < counts[0]).astype(F32)

    def gradients(all_values, name):
        ga_out, gc_out, gb_out = [box(name + mode + "_in")[0] for mode in "acb"]
        parts = [two(values) for values in all_values]
        cols = jnp.zeros((64, 128), F32)
        lanes = iota((64, 128), 1)
        for t in range(T):
            raw = mm_two(tb2[t], parts[t], 1)
            pack(t, raw * depth[t], ga_out)
            col = jnp.sum(ta[t] * raw, axis=1, keepdims=True)
            cols = jnp.where(lanes == t, col, cols)
        send(name + "a_in")
        for t in range(T):
            pack(t, mm_two(tac2[t], parts[t]), gb_out)
        send(name + "b_in")
        tile = jnp.transpose(jnp.concatenate([cols, jnp.zeros((64, 128), F32)], axis=0))[:4]
        return tile, gc_out

    all_values = []
    for t in range(T):
        high, low = two(jnp.transpose(ta[t]))
        at2[t, 0:128] = high
        at2[t, 128:256] = low
        high, low = two(ta[t] * depth[t])
        tac2[t, 0:64] = high
        tac2[t, 64:128] = low
        model = mm_two(at2[t], (bc_high[t], bc_low[t]))
        all_values.append((data[t].astype(F32) - model) * live(t))
    tile, gc_out = gradients(all_values, "g")
    for j in range(G):
        gc_out[j] = tile
    send("gc_in")
    for t in range(T):
        left[t, :, 64:128] = at2[t]

    def fold(w, src, v):
        rows = src.reshape(256, 128)
        parts = three(rows)
        v[...] = mm(w[...], parts[0:256]) + (mm(w[...], parts[256:512]) + mm(w[...], parts[512:768]))
        return v[...]

    def blend(src):
        both = mm(mix[...], three(stacked(src)))
        return jnp.where(iota((128, 128), 1) < 64, both[:128], pltpu.roll(both[128:], 64, 1))

    src = arrived("gb_in")
    serve(wbt, fold(wb, src[...], gb), "gb_out")
    src = arrived("ga_in")
    serve(wat, fold(wa, src[...], ga), "ga_out")
    src = arrived("gc_in")
    box("gc_out")[0][...] = blend(src).reshape(G, 8, 128)
    send("gc_out")

    def direction(name):
        src = arrived(name + "b_out")
        unpack(src, db)
        src = arrived(name + "c_out")
        total = jnp.sum(src[...], axis=0)
        du = columns(jnp.transpose(total))
        rights = []
        for t in range(T):
            high, low = two(db[t] * depth[t] + tb[t] * du[t])
            rights.append((
                jnp.concatenate([bc_high[t], high], axis=0),
                jnp.concatenate([bc_low[t], low], axis=0),
            ))
        src = arrived(name + "a_out")
        unpack(src, da)
        products = []
        for t in range(T):
            high, low = two(jnp.transpose(da[t]))
            left[t, 0:128, 0:64] = high
            left[t, 128:256, 0:64] = low
            products.append(mm_two(left[t], rights[t]) * live(t))
        return total, products

    def norm(value):
        return jnp.sum(value, axis=(0, 1), keepdims=True)

    total_g, products = direction("g")
    tile, gc_out = gradients(products, "w")
    squares = jnp.zeros((128, 128), F32)
    for t in range(T):
        jg[t] = products[t]
        squares = squares + products[t] * products[t]
    own_g = total_g[:, 0:64]
    g_part = norm(ga[...] * ga[...]) + norm(gb[...] * gb[...]) + norm(own_g * own_g)
    j_part = norm(squares)
    row4, lane4 = iota((4, 128), 0), iota((4, 128), 1)
    tile = jnp.where((row4 == 0) & (lane4 >= 64), g_part, tile)
    tile = jnp.where((row4 == 1) & (lane4 >= 64), j_part, tile)
    for j in range(G):
        gc_out[j] = tile
    send("wc_in")

    src = arrived("wb_in")
    serve(wbt, fold(wb, src[...], vb), "wb_out")
    src = arrived("wa_in")
    serve(wat, fold(wa, src[...], va), "wa_out")
    src = arrived("wc_in")
    group = jnp.sum(src[...], axis=0)
    u = blend(src)
    down, across = iota((128, 128), 0), iota((128, 128), 1)
    u = jnp.where(across >= 64, jnp.where(down % 8 == 4, group[0:1, 127:128], u), u)
    u = jnp.where(across >= 64, jnp.where(down % 8 == 5, group[1:2, 127:128], u), u)
    box("wc_out")[0][...] = u.reshape(G, 8, 128)
    send("wc_out")

    a_put, b_put = box("a_put")[0], box("b_put")[0]
    for j in range(G):
        a_put[j, 0:4] = ga[4 * j:4 * j + 4]
        a_put[j, 4:8] = va[4 * j:4 * j + 4]
        b_put[j, 0:4] = gb[4 * j:4 * j + 4]
        b_put[j, 4:8] = vb[4 * j:4 * j + 4]
    send("a_put")
    send("b_put")

    total_w, products = direction("w")
    lam = damp[0]
    g_norm = total_w[4:5, 127:128]
    j_norm = total_w[5:6, 127:128]
    alpha0 = g_norm / (j_norm + lam * g_norm)

    def residual_of(g, w):
        return g - alpha0 * (w + lam * g)

    own_w = total_w[:, 0:64]
    r_a = residual_of(ga[...], va[...])
    r_b = residual_of(gb[...], vb[...])
    r_c = residual_of(own_g, own_w)
    rr_part = norm(r_a * r_a + r_b * r_b) + norm(r_c * r_c)
    rg_part = norm(r_a * ga[...] + r_b * gb[...]) + norm(r_c * own_g)
    square = jnp.zeros((128, 128), F32)
    cross = jnp.zeros((128, 128), F32)
    for t in range(T):
        jr = residual_of(jg[t], products[t])
        square = square + jr * jr
        cross = cross + jr * jg[t]

    parts = (rr_part, rg_part, norm(square), norm(cross))
    row = zero_row
    for i, part in enumerate(parts):
        row = jnp.where(lane // 32 == i, part, row)
    out = box("sum_col")[0]
    for j in range(G):
        out[j] = row
    send("sum_col")
    src = arrived("sum_col")
    row = jnp.sum(src[...], axis=0)
    out = box("sum_row")[0]
    for j in range(G):
        out[j] = row
    send("sum_row")
    src_a = arrived("a_put")
    src_b = arrived("b_put")
    src = arrived("sum_row")
    row = jnp.sum(src[...], axis=0)
    r_norm, r_g, jr_norm, jr_jg = [row[:, 32 * i:32 * i + 1] for i in range(4)]
    beta = r_norm / g_norm
    curve = (
        jr_norm + lam * r_norm
        + 2.0 * beta * (jr_jg + lam * r_g)
        + beta * beta * (j_norm + lam * g_norm)
    )
    alpha1 = r_norm / curve

    def step(g, w):
        return alpha0 * g + alpha1 * (residual_of(g, w) + beta * g)

    for j in range(G):
        out_a[4 * j:4 * j + 4] = step(src_a[j, 0:4], src_a[j, 4:8])
        out_b[4 * j:4 * j + 4] = step(src_b[j, 0:4], src_b[j, 4:8])
    out_c[...] = step(own_g, own_w)
    for i in range(n):
        wait(send_sem.at[i], outbox[i])


def put(a, b, c, x, y, z):
    x[...] = a[...]
    y[...] = b[...]
    z[...] = c[...]


def per_device(
    tile_data, tile_coords, tile_counts, factor_rows, factor_cols, factor_depth, damping
):
    vmem = pl.BlockSpec(memory_space=pltpu.VMEM)
    boxes = [pltpu.VMEM((G, rows, 128), F32) for _, _, rows in EXCHANGES]
    blocks = ((64, 128), (64, 128), (8, 64))
    steps = pl.pallas_call(
        kernel,
        out_shape=tuple(pltpu.VMEM(block, F32) for block in blocks),
        in_specs=[pl.BlockSpec(memory_space=pltpu.HBM)] * 7,
        out_specs=(vmem, vmem, vmem),
        scratch_shapes=[
            *boxes, *boxes,
            pltpu.SMEM((3, T), jnp.int32), pltpu.SMEM((1,), jnp.int32), pltpu.SMEM((1,), F32),
            pltpu.VMEM((64, 128), F32), pltpu.VMEM((64, 128), F32), pltpu.VMEM((8, 64), F32),
            pltpu.VMEM((T, 128, 128), BF16),
            *[pltpu.VMEM((64, 128), F32)] * 4,
            *[pltpu.VMEM((T, 64, 128), F32)] * 4,
            pltpu.VMEM((T, 128, 128), F32),
            pltpu.VMEM((T, 256, 64), BF16),
            pltpu.VMEM((T, 128, 128), BF16), pltpu.VMEM((T, 128, 128), BF16),
            pltpu.VMEM((T, 64, 128), BF16), pltpu.VMEM((T, 64, 128), BF16),
            pltpu.VMEM((T, 256, 128), BF16),
            pltpu.VMEM((64, 128), F32),
            pltpu.VMEM((64, 256), BF16), pltpu.VMEM((64, 256), BF16),
            pltpu.VMEM((256, 192), BF16), pltpu.VMEM((256, 192), BF16),
            pltpu.VMEM((256, 192), BF16),
            pltpu.SemaphoreType.DMA((7,)),
            pltpu.SemaphoreType.DMA((len(EXCHANGES),)),
            pltpu.SemaphoreType.DMA((len(EXCHANGES),)),
        ],
        compiler_params=pltpu.CompilerParams(collective_id=0, has_side_effects=True),
        name="gauss_newton",
    )(
        tile_coords, tile_counts, damping.reshape(1),
        factor_rows, factor_cols, factor_depth.T, tile_data,
    )
    step_a, step_b, step_c = pl.pallas_call(
        put,
        out_shape=tuple(jax.ShapeDtypeStruct(block, F32) for block in blocks),
        in_specs=[vmem, vmem, vmem],
        out_specs=(vmem, vmem, vmem),
        name="put",
    )(*[pltpu.with_memory_space_constraint(step, pltpu.VMEM) for step in steps])
    return step_a, step_b, step_c.T


def solution(mesh):
    both = ("row", "col")
    flip = ("col", "row")
    return jax.shard_map(
        per_device,
        mesh=mesh,
        in_specs=(
            P(both, None, None), P(None, both), P(both),
            P(None, both), P(None, flip), P(None, both), P(),
        ),
        out_specs=(P(None, both), P(None, flip), P(None, both)),
        check_vma=False,
    )
```

```python
import jax
import jax.numpy as jnp
from jax import lax
from jax.experimental import pallas as pl
from jax.experimental.pallas import tpu as pltpu
from jax.sharding import PartitionSpec as P

G = 16
T = 4
RS = 4
F32 = jnp.float32
BF16 = jnp.bfloat16

COL_PEERS = [(dz, dc) for dz in (4, 3, 5, 2, 6, 1, 7) for dc in (0, 1)] + [(0, 1)]
ROW_PEERS = sorted(
    [(dy, dx) for dy in range(4) for dx in range(4) if (dy, dx) != (0, 0)],
    key=lambda d: -(min(d[0], 4 - d[0]) + min(d[1], 4 - d[1])),
)

PARTS = 1
SLOTS = [tuple(range(T // PARTS * i, T // PARTS * (i + 1))) for i in range(PARTS)]


def slot_boxes(name):
    return [(name + str(i), 0, 16 // PARTS) for i in range(PARTS)]


EXCHANGES = (
    ("a_slices", 0, 8), ("c_own", 1, 4), ("b_slices", 1, 8),
    *slot_boxes("a_slots"), ("b_slots", 1, 16), ("c_slots", 0, 4),
    *slot_boxes("ga_in"), ("gc_in", 1, 4), ("gb_in", 1, 16),
    *slot_boxes("ga_out"), ("gb_out", 1, 16), ("gc_out", 0, 4),
    *slot_boxes("wa_in"), ("wc_in", 1, 4), ("wb_in", 1, 16),
    *slot_boxes("wa_out"), ("wb_out", 1, 16), ("wc_out", 0, 4),
    ("a_put", 0, 8), ("b_put", 1, 8), ("c_put", 0, 8),
    ("sum_col", 0, 1), ("sum_row", 1, 1),
)
INDEX = {name: i for i, (name, _, _) in enumerate(EXCHANGES)}


def mm(a, b, rhs_dim=0):
    return lax.dot_general(a, b, (((1,), (rhs_dim,)), ((), ())), preferred_element_type=F32)


def split(x, count, axis):
    parts = []
    for _ in range(count):
        part = x.astype(BF16)
        parts.append(part)
        x = x - part.astype(F32)
    return parts if axis is None else jnp.concatenate(parts, axis=axis)


def left_of(x, axis=1):
    high, low = split(x, 2, None)
    return jnp.concatenate([high, high, low], axis=axis)


def right_of(x, axis):
    high, low = split(x, 2, None)
    return jnp.concatenate([high, low, high], axis=axis)


def iota(shape, dim):
    return lax.broadcasted_iota(jnp.int32, shape, dim)


def kernel(coords_hbm, counts_hbm, damp_hbm, fa_hbm, fb_hbm, fc_hbm, data_hbm, *refs):
    out_a, out_b, out_c = refs[:3]
    refs = refs[3:]
    n = len(EXCHANGES)
    outbox, inbox = refs[:n], refs[n:2 * n]
    (
        coords, counts, damp, fa, fb, fc, data,
        va, vb, ga, gb, ta, tb, da, db, jg,
        at3, tb3, tac3, bc3, left, xc,
        wa, wb, wat, wbt, same_a, same_b, mix, load_sem, send_sem, recv_sem,
    ) = refs[2 * n:]
    p = lax.axis_index("row")
    q = lax.axis_index("col")
    z, core = q // 2, q % 2
    col_of = [((z + dz) % 8) * 2 + (core + dc) % 2 for dz, dc in COL_PEERS]
    y, x = p // 4, p % 4
    row_of = [((y + dy) % 4) * 4 + (x + dx) % 4 for dy, dx in ROW_PEERS]

    barrier = pltpu.get_barrier_semaphore()
    for peer in col_of:
        pl.semaphore_signal(barrier, inc=1, device_id={"col": peer})
    for peer in row_of:
        pl.semaphore_signal(barrier, inc=1, device_id={"row": peer})

    loads = [
        pltpu.make_async_copy(src, dst, load_sem.at[i])
        for i, (src, dst) in enumerate((
            (coords_hbm, coords), (counts_hbm, counts), (damp_hbm, damp),
            (fa_hbm, fa), (fb_hbm, fb), (fc_hbm, fc), (data_hbm, data),
        ))
    ]
    for load in loads:
        load.start()

    def box(name):
        return outbox[INDEX[name]], inbox[INDEX[name]]

    def send(name):
        i = INDEX[name]
        me, peers, axis = ((q, col_of, "col"), (p, row_of, "row"))[EXCHANGES[i][1]]
        src, dst = outbox[i], inbox[i]
        for peer in peers:
            pltpu.make_async_remote_copy(
                src_ref=src.at[peer],
                dst_ref=dst.at[me],
                send_sem=send_sem.at[i],
                recv_sem=recv_sem.at[i],
                device_id={axis: peer},
            ).start()
        dst[me] = src[me]

    def wait(sem, ref):
        some = ref.at[pl.ds(0, G - 1)]
        pltpu.make_async_copy(some, some, sem).wait()

    def arrived(name):
        i = INDEX[name]
        wait(recv_sem.at[i], inbox[i])
        return inbox[i]

    lane = iota((1, 128), 1)
    zero_row = jnp.zeros((1, 128), F32)

    def positions(coord_row, member, groups):
        wide = 16 // len(groups)
        lanes = iota((1, 256), 1)
        val = jnp.zeros((1, 256), F32)
        for g, slots in enumerate(groups):
            for i, t in enumerate(slots):
                here = lanes - (256 // len(groups) * g + member * wide + RS * i)
                at = (here >= 0) & (here < RS)
                val = jnp.where(at, (coords[coord_row, t] * RS + here).astype(F32), val)
        return val[:, 0:128], val[:, 128:256]

    def depth_index(member):
        here = lane - member * 8
        val = zero_row
        for t in range(T):
            at = (here == t) | (here == t + T)
            val = jnp.where(at, coords[2, t].astype(F32), val)
        return val

    loads[0].wait()
    first, second = positions(0, q, SLOTS)
    info_col = jnp.concatenate([first, second, depth_index(q), zero_row], axis=0)
    first, second = positions(1, p, [range(T)])
    info_row = jnp.concatenate([first, second, depth_index(p), zero_row], axis=0)
    for load in loads[3:6]:
        load.wait()
    own = jnp.concatenate([fc[0:4], fc[4:8]], axis=1)
    a_slices, c_own, b_slices = box("a_slices")[0], box("c_own")[0], box("b_slices")[0]
    for j in range(G):
        a_slices[j, 0:4] = fa[4 * j:4 * j + 4]
        a_slices[j, 4:8] = info_col
        c_own[j] = own
        b_slices[j, 0:4] = fb[4 * j:4 * j + 4]
        b_slices[j, 4:8] = info_row

    pl.semaphore_wait(barrier, 2 * (G - 1))
    send("a_slices")
    send("b_slices")
    send("c_own")

    def across_of(info):
        return jnp.concatenate([info[4:5], info[5:6]], axis=1).astype(jnp.int32)

    lane64 = iota((128, 192), 1) % 64

    def back_matrix(info, dst):
        turned = jnp.transpose(info).astype(jnp.int32)
        for half in range(2):
            here = turned[:, 4 + half:5 + half]
            dst[128 * half:128 * half + 128] = (lane64 == here).astype(BF16)
        return turned

    def names_of(name):
        return [name + str(i) for i in range(PARTS)]

    def serve_blocks(w, v, names):
        parts = split(v, 3, 0)
        size = 256 // len(names)
        for i, name in enumerate(names):
            total = mm(w[size * i:size * i + size], parts)
            box(name)[0][...] = total.reshape(G, -1, 128)
            send(name)

    def serve(same, rows, names):
        high, mid, low = split(rows, 3, None)
        most = jnp.concatenate([high, mid], axis=1)
        size = 256 // len(names)
        for i, name in enumerate(names):
            w = same[size * i:size * i + size]
            both = mm(w, most)
            total = both[:, 0:128] + (both[:, 128:256] + mm(w, low))
            box(name)[0][...] = total.reshape(G, -1, 128)
            send(name)

    def rows_of(names):
        boxes = [arrived(name) for name in names]
        return jnp.concatenate([ref[...].reshape(-1, 128) for ref in boxes], axis=0)

    def stacked(src):
        for j in range(G):
            xc[4 * j:4 * j + 4] = src[j]
        return xc[...]

    src = arrived("b_slices")
    info_row = jnp.sum(src[...], axis=0)
    turned_row = back_matrix(info_row, wbt)
    for j in range(G):
        vb[4 * j:4 * j + 4] = src[j, 0:4]
    serve_blocks(wbt, vb[...], ["b_slots"])
    columns_here = split(stacked(arrived("c_own")), 3, 0)
    src = arrived("a_slices")
    info_col = jnp.sum(src[...], axis=0)
    turned_col = back_matrix(info_col, wat)
    k_there = turned_col[:, 6:7]
    down, lane64 = iota((128, 192), 0), iota((128, 192), 1) % 64
    column = (lane64 // 4) * 128 + q * 8 + lane64 % 4
    wanted = jnp.where(down % 8 < T, k_there, -1)
    pick = jnp.concatenate(
        [(wanted == column).astype(BF16), (wanted == column + 4).astype(BF16)], axis=0
    )
    both = mm(pick, columns_here)
    c_out = box("c_slots")[0]
    c_out[...] = (pltpu.roll(both[:128], 64, 1) + both[128:]).reshape(G, 8, 128)[:, 0:4]
    send("c_slots")
    for j in range(G):
        va[4 * j:4 * j + 4] = src[j, 0:4]
    serve_blocks(wat, va[...], names_of("a_slots"))

    for info, turn, w, same in (
        (info_col, turned_col, wa, same_a), (info_row, turned_row, wb, same_b)
    ):
        across = across_of(info)
        w[...] = (iota((64, 256), 0) == across).astype(BF16)
        for half in range(2):
            here = turn[:, 4 + half:5 + half]
            same[128 * half:128 * half + 128] = (
                jnp.broadcast_to(across, (128, 256)) == here
            ).astype(BF16)

    spread = (iota((128, 192), 0) == (lane64 // 4) * 8 + lane64 % 4).astype(BF16)
    k_tiles = jnp.broadcast_to(info_row[6:7], (8, 128))
    k_lane = mm(split(k_tiles, 3, 1), jnp.concatenate([spread, spread, spread], axis=0))
    k_lane = jnp.broadcast_to(k_lane[0:1].astype(jnp.int32), (128, 192))
    mix[0:128] = (k_lane == p * 128 + down).astype(BF16)
    mix[128:256] = (k_lane == wanted).astype(BF16)

    def unpack(src, dst, slots):
        for i, t in enumerate(slots):
            for j in range(G):
                dst[t, 4 * j:4 * j + 4] = src[j, 4 * i:4 * i + 4]

    def pack(i, value, dst):
        for j in range(G):
            dst[j, 4 * i:4 * i + 4] = value[4 * j:4 * j + 4]

    def turned_of(rows):
        return jnp.transpose(jnp.concatenate([rows, jnp.zeros((4, 128), F32)], axis=0))

    def columns(turned):
        return [jnp.broadcast_to(turned[64:128, t:t + 1], (64, 128)) for t in range(T)]

    src = arrived("b_slots")
    unpack(src, tb, range(T))
    for t in range(T):
        tb3[t] = left_of(tb[t])
    src = arrived("c_slots")
    depth = columns(turned_of(jnp.sum(src[...], axis=0)))
    for t in range(T):
        bc3[t] = right_of(tb[t] * depth[t], 0)
    for load in (loads[1], loads[2], loads[6]):
        load.wait()

    def norm(value):
        return jnp.sum(value, axis=(0, 1), keepdims=True)

    def live(t):
        return (t < counts[0]).astype(F32)

    def gradients(values_of, name, scalars_of):
        gc_out, gb_out = box(name + "c_in")[0], box(name + "b_in")[0]
        cols = jnp.zeros((64, 128), F32)
        lanes = iota((64, 128), 1)
        for number, slots in enumerate(SLOTS):
            parts = [split(values, 2, None) for values in values_of(number, slots)]
            ga_name = name + "a_in" + str(number)
            for i, t in enumerate(slots):
                high, low = parts[i]
                raw = mm(tb3[t], jnp.concatenate([high, low, high], axis=1), 1)
                pack(i, raw * depth[t], box(ga_name)[0])
                col = jnp.sum(ta[t] * raw, axis=1, keepdims=True)
                cols = jnp.where(lanes == t, col, cols)
            send(ga_name)
            if slots[-1] == T - 1:
                tile = jnp.transpose(jnp.concatenate([cols, jnp.zeros((64, 128), F32)], axis=0))[:4]
                row4, lane4 = iota((4, 128), 0), iota((4, 128), 1)
                for i, scalar in enumerate(scalars_of()):
                    tile = jnp.where((row4 == i) & (lane4 >= 64), scalar, tile)
                for j in range(G):
                    gc_out[j] = tile
                send(name + "c_in")
            for i, t in enumerate(slots):
                high, low = parts[i]
                pack(t, mm(tac3[t], jnp.concatenate([high, low, high], axis=0)), gb_out)
        send(name + "b_in")
        return cols

    def data_left(number, slots):
        src = arrived("a_slots" + str(number))
        unpack(src, ta, slots)
        values = []
        for t in slots:
            at3[t] = left_of(jnp.transpose(ta[t]))
            tac3[t] = left_of(ta[t] * depth[t])
            values.append((data[t].astype(F32) - mm(at3[t], bc3[t])) * live(t))
        return values

    cols_g = gradients(data_left, "g", lambda: ())
    for t in range(T):
        for part in range(3):
            left[t, :, 128 * part + 64:128 * part + 128] = at3[t, :, 64 * part:64 * part + 64]

    def fold(w, rows, v):
        high, mid, low = split(rows, 3, None)
        most = mm(w[...], jnp.concatenate([high, mid], axis=1))
        v[...] = most[:, 0:128] + (most[:, 128:256] + mm(w[...], low))

    def blend(src):
        both = mm(mix[...], split(stacked(src), 3, 0))
        return jnp.where(iota((128, 128), 1) < 64, both[:128], pltpu.roll(both[128:], 64, 1))

    lane_col = iota((1, 1, 128), 2)

    def send_sums(name, u, base, scalars):
        own = pltpu.roll(u, 64, 1).reshape(G, 8, 128)
        u = u.reshape(G, 8, 128)
        c_put[:, base:base + 4] = jnp.where(lane_col < 64, u[:, 0:4], own[:, 4:8])
        now = u[:, 0:4]
        for i, scalar in enumerate(scalars):
            at = (iota((1, 4, 128), 1) == i) & (iota((1, 4, 128), 2) < 64)
            now = jnp.where(at, jnp.broadcast_to(scalar.reshape(1, 1, 1), (1, 4, 128)), now)
        box(name + "c_out")[0][...] = now
        send(name + "c_out")

    c_put = box("c_put")[0]

    src = arrived("gc_in")
    send_sums("g", blend(src), 0, ())
    rows_b = rows_of(["gb_in"])
    serve(same_b, rows_b, ["gb_out"])
    rows_a = rows_of(names_of("ga_in"))
    serve(same_a, rows_a, names_of("ga_out"))
    fold(wb, rows_b, gb)
    fold(wa, rows_a, ga)
    g_part = norm(ga[...] * ga[...] + gb[...] * gb[...])

    def direction_bc(name):
        src = arrived(name + "b_out")
        unpack(src, db, range(T))
        src = arrived(name + "c_out")
        total = jnp.sum(src[...], axis=0)
        turned = turned_of(total)
        du = columns(turned)
        rights = []
        for t in range(T):
            high, low = split(db[t] * depth[t] + tb[t] * du[t], 2, None)
            rights.append(jnp.concatenate(
                [bc3[t, 0:64], high, bc3[t, 64:128], low, bc3[t, 0:64], high], axis=0
            ))
        return total, turned[64:128], rights

    def direction_a(name, rights, number, slots):
        src = arrived(name + "a_out" + str(number))
        unpack(src, da, slots)
        products = []
        for t in slots:
            high, low = split(jnp.transpose(da[t]), 2, None)
            left[t, :, 0:64] = high
            left[t, :, 128:192] = high
            left[t, :, 256:320] = low
            products.append(mm(left[t], rights[t]) * live(t))
        return products

    _, dirs_g, rights = direction_bc("g")
    g_part = g_part + norm(cols_g[:, 0:8] * dirs_g)

    def second_values(number, slots):
        products = direction_a("g", rights, number, slots)
        for t, product in zip(slots, products):
            jg[t] = product
        return products

    def first_scalars():
        squares = jnp.zeros((128, 128), F32)
        for t in range(T):
            squares = squares + jg[t] * jg[t]
        return g_part, norm(squares)

    cols_w = gradients(second_values, "w", first_scalars)

    src = arrived("wc_in")
    group = jnp.sum(src[...], axis=0)
    send_sums("w", blend(src), 4, (group[0:1, 127:128], group[1:2, 127:128]))
    rows_b = rows_of(["wb_in"])
    serve(same_b, rows_b, ["wb_out"])
    rows_a = rows_of(names_of("wa_in"))
    serve(same_a, rows_a, names_of("wa_out"))
    fold(wb, rows_b, vb)
    fold(wa, rows_a, va)
    total_w, dirs_w, rights = direction_bc("w")
    lam = damp[0]
    g_norm = total_w[0:1, 0:1]
    j_norm = total_w[1:2, 0:1]
    alpha0 = g_norm / (j_norm + lam * g_norm)

    def residual_of(g, w):
        return g - alpha0 * (w + lam * g)

    r_a = residual_of(ga[...], va[...])
    r_b = residual_of(gb[...], vb[...])
    r_cols = residual_of(cols_g[:, 0:8], cols_w[:, 0:8])
    rr_part = norm(r_a * r_a + r_b * r_b) + norm(r_cols * residual_of(dirs_g, dirs_w))
    rg_part = norm(r_a * ga[...] + r_b * gb[...]) + norm(r_cols * dirs_g)
    square = jnp.zeros((128, 128), F32)
    cross = jnp.zeros((128, 128), F32)
    for number, slots in enumerate(SLOTS):
        for t, product in zip(slots, direction_a("w", rights, number, slots)):
            jr = residual_of(jg[t], product)
            square = square + jr * jr
            cross = cross + jr * jg[t]

    parts = (rr_part, rg_part, norm(square), norm(cross))
    row = zero_row
    for i, part in enumerate(parts):
        row = jnp.where(lane // 32 == i, part, row)
    out = box("sum_col")[0]
    for j in range(G):
        out[j] = row
    send("sum_col")
    a_put, b_put = box("a_put")[0], box("b_put")[0]
    for j in range(G):
        a_put[j, 0:4] = ga[4 * j:4 * j + 4]
        a_put[j, 4:8] = va[4 * j:4 * j + 4]
        b_put[j, 0:4] = gb[4 * j:4 * j + 4]
        b_put[j, 4:8] = vb[4 * j:4 * j + 4]
    send("a_put")
    send("b_put")
    send("c_put")

    src = arrived("sum_col")
    row = jnp.sum(src[...], axis=0)
    out = box("sum_row")[0]
    for j in range(G):
        out[j] = row
    send("sum_row")
    src_a = arrived("a_put")
    src_b = arrived("b_put")
    own = jnp.sum(arrived("c_put")[...], axis=0)
    own_g = jnp.concatenate([own[0:4, 0:64], own[0:4, 64:128]], axis=0)
    own_w = jnp.concatenate([own[4:8, 0:64], own[4:8, 64:128]], axis=0)
    for j in range(G):
        ga[4 * j:4 * j + 4] = src_a[j, 0:4]
        va[4 * j:4 * j + 4] = src_a[j, 4:8]
        gb[4 * j:4 * j + 4] = src_b[j, 0:4]
        vb[4 * j:4 * j + 4] = src_b[j, 4:8]
    blocks = ((ga[...], va[...], out_a), (gb[...], vb[...], out_b), (own_g, own_w, out_c))
    bases = [(alpha0 * g, residual_of(g, w), g, out) for g, w, out in blocks]
    src = arrived("sum_row")
    row = jnp.sum(src[...], axis=0)
    r_norm, r_g, jr_norm, jr_jg = [row[:, 32 * i:32 * i + 1] for i in range(4)]
    beta = r_norm / g_norm
    curve = (
        jr_norm + lam * r_norm
        + 2.0 * beta * (jr_jg + lam * r_g)
        + beta * beta * (j_norm + lam * g_norm)
    )
    alpha1 = r_norm / curve

    for base, r, g, out in bases:
        out[...] = base + alpha1 * (r + beta * g)
    for i in range(n):
        wait(send_sem.at[i], outbox[i])


def put(a, b, c, x, y, z):
    x[...] = a[...]
    y[...] = b[...]
    z[...] = c[...]


def per_device(
    tile_data, tile_coords, tile_counts, factor_rows, factor_cols, factor_depth, damping
):
    vmem = pl.BlockSpec(memory_space=pltpu.VMEM)
    boxes = [pltpu.VMEM((G, rows, 128), F32) for _, _, rows in EXCHANGES]
    blocks = ((64, 128), (64, 128), (8, 64))
    steps = pl.pallas_call(
        kernel,
        out_shape=tuple(pltpu.VMEM(block, F32) for block in blocks),
        in_specs=[pl.BlockSpec(memory_space=pltpu.HBM)] * 7,
        out_specs=(vmem, vmem, vmem),
        scratch_shapes=[
            *boxes, *boxes,
            pltpu.SMEM((3, T), jnp.int32), pltpu.SMEM((1,), jnp.int32), pltpu.SMEM((1,), F32),
            pltpu.VMEM((64, 128), F32), pltpu.VMEM((64, 128), F32), pltpu.VMEM((8, 64), F32),
            pltpu.VMEM((T, 128, 128), BF16),
            *[pltpu.VMEM((64, 128), F32)] * 4,
            *[pltpu.VMEM((T, 64, 128), F32)] * 4,
            pltpu.VMEM((T, 128, 128), F32),
            pltpu.VMEM((T, 128, 192), BF16),
            pltpu.VMEM((T, 64, 384), BF16), pltpu.VMEM((T, 64, 384), BF16),
            pltpu.VMEM((T, 192, 128), BF16),
            pltpu.VMEM((T, 128, 384), BF16),
            pltpu.VMEM((64, 128), F32),
            pltpu.VMEM((64, 256), BF16), pltpu.VMEM((64, 256), BF16),
            pltpu.VMEM((256, 192), BF16), pltpu.VMEM((256, 192), BF16),
            pltpu.VMEM((256, 256), BF16), pltpu.VMEM((256, 256), BF16),
            pltpu.VMEM((256, 192), BF16),
            pltpu.SemaphoreType.DMA((7,)),
            pltpu.SemaphoreType.DMA((len(EXCHANGES),)),
            pltpu.SemaphoreType.DMA((len(EXCHANGES),)),
        ],
        compiler_params=pltpu.CompilerParams(collective_id=0, has_side_effects=True),
        name="gauss_newton",
    )(
        tile_coords, tile_counts, damping.reshape(1),
        factor_rows, factor_cols, factor_depth.T, tile_data,
    )
    step_a, step_b, step_c = pl.pallas_call(
        put,
        out_shape=tuple(jax.ShapeDtypeStruct(block, F32) for block in blocks),
        in_specs=[vmem, vmem, vmem],
        out_specs=(vmem, vmem, vmem),
        name="put",
    )(*[pltpu.with_memory_space_constraint(step, pltpu.VMEM) for step in steps])
    return step_a, step_b, step_c.T


def solution(mesh):
    both = ("row", "col")
    flip = ("col", "row")
    return jax.shard_map(
        per_device,
        mesh=mesh,
        in_specs=(
            P(both, None, None), P(None, both), P(both),
            P(None, both), P(None, flip), P(None, both), P(),
        ),
        out_specs=(P(None, both), P(None, flip), P(None, both)),
        check_vma=False,
    )
```

```python
import jax
import jax.numpy as jnp
from jax import lax
from jax.experimental import pallas as pl
from jax.experimental.pallas import tpu as pltpu
from jax.sharding import PartitionSpec as P

G = 16
T = 4
RS = 4
F32 = jnp.float32
BF16 = jnp.bfloat16

def ring(d, size):
    return min(d, size - d)


COL_PEERS = sorted(
    [(dz, dc) for dz in range(8) for dc in range(2) if (dz, dc) != (0, 0)],
    key=lambda d: (-(ring(d[0], 8) + d[1]) if d[0] else 0, -d[1], d[0]),
)
ROW_PEERS = sorted(
    [(dy, dx) for dy in range(4) for dx in range(4) if (dy, dx) != (0, 0)],
    key=lambda d: (-(ring(d[0], 4) + ring(d[1], 4)), -ring(d[0], 4)),
)

PARTS = 1
SLOTS = [tuple(range(T // PARTS * i, T // PARTS * (i + 1))) for i in range(PARTS)]


def slot_boxes(name):
    return [(name + str(i), 0, 16 // PARTS) for i in range(PARTS)]


EXCHANGES = (
    ("a_slices", 0, 8), ("c_own", 1, 4), ("b_slices", 1, 8),
    *slot_boxes("a_slots"), ("b_slots", 1, 16), ("c_slots", 0, 4),
    *slot_boxes("ga_in"), ("gc_in", 1, 4), ("gb_in", 1, 16),
    *slot_boxes("ga_out"), ("gb_out", 1, 16), ("gc_out", 0, 4),
    *slot_boxes("wa_in"), ("wc_in", 1, 4), ("wb_in", 1, 16),
    *slot_boxes("wa_out"), ("wb_out", 1, 16), ("wc_out", 0, 4),
    ("a_put", 0, 8), ("b_put", 1, 8), ("c_put", 0, 8),
    ("sum_col", 0, 1), ("sum_row", 1, 1),
)
INDEX = {name: i for i, (name, _, _) in enumerate(EXCHANGES)}


def mm(a, b, rhs_dim=0):
    return lax.dot_general(a, b, (((1,), (rhs_dim,)), ((), ())), preferred_element_type=F32)


def split(x, count, axis):
    parts = []
    for _ in range(count):
        part = x.astype(BF16)
        parts.append(part)
        x = x - part.astype(F32)
    return parts if axis is None else jnp.concatenate(parts, axis=axis)


def left_of(x, axis=1):
    high, low = split(x, 2, None)
    return jnp.concatenate([high, high, low], axis=axis)


def right_of(x, axis):
    high, low = split(x, 2, None)
    return jnp.concatenate([high, low, high], axis=axis)


def iota(shape, dim):
    return lax.broadcasted_iota(jnp.int32, shape, dim)


def kernel(coords_hbm, counts_hbm, damp_hbm, fa_hbm, fb_hbm, fc_hbm, data_hbm, *refs):
    out_a, out_b, out_c = refs[:3]
    refs = refs[3:]
    n = len(EXCHANGES)
    outbox, inbox = refs[:n], refs[n:2 * n]
    (
        coords, counts, damp, fa, fb, fc, data,
        va, vb, ga, gb, ta, tb, da, db, jg,
        bct3, tb3, tac3, a3, left, datat, xc,
        wa, wb, wat, wbt, same_a, same_b, mix, load_sem, send_sem, recv_sem,
    ) = refs[2 * n:]
    p = lax.axis_index("row")
    q = lax.axis_index("col")
    z, core = q // 2, q % 2
    col_of = [((z + dz) % 8) * 2 + (core + dc) % 2 for dz, dc in COL_PEERS]
    y, x = p // 4, p % 4
    row_of = [((y + dy) % 4) * 4 + (x + dx) % 4 for dy, dx in ROW_PEERS]

    barrier = pltpu.get_barrier_semaphore()
    for peer in col_of:
        pl.semaphore_signal(barrier, inc=1, device_id={"col": peer})
    for peer in row_of:
        pl.semaphore_signal(barrier, inc=1, device_id={"row": peer})

    loads = [
        pltpu.make_async_copy(src, dst, load_sem.at[i])
        for i, (src, dst) in enumerate((
            (coords_hbm, coords), (counts_hbm, counts), (damp_hbm, damp),
            (fa_hbm, fa), (fb_hbm, fb), (fc_hbm, fc), (data_hbm, data),
        ))
    ]
    for load in loads:
        load.start()

    def box(name):
        return outbox[INDEX[name]], inbox[INDEX[name]]

    def send(name):
        i = INDEX[name]
        me, peers, axis = ((q, col_of, "col"), (p, row_of, "row"))[EXCHANGES[i][1]]
        src, dst = outbox[i], inbox[i]
        for peer in peers:
            pltpu.make_async_remote_copy(
                src_ref=src.at[peer],
                dst_ref=dst.at[me],
                send_sem=send_sem.at[i],
                recv_sem=recv_sem.at[i],
                device_id={axis: peer},
            ).start()
        dst[me] = src[me]

    def wait(sem, ref):
        some = ref.at[pl.ds(0, G - 1)]
        pltpu.make_async_copy(some, some, sem).wait()

    def arrived(name):
        i = INDEX[name]
        wait(recv_sem.at[i], inbox[i])
        return inbox[i]

    lane = iota((1, 128), 1)
    zero_row = jnp.zeros((1, 128), F32)

    def positions(coord_row, member, groups):
        wide = 16 // len(groups)
        lanes = iota((1, 256), 1)
        val = jnp.zeros((1, 256), F32)
        for g, slots in enumerate(groups):
            for i, t in enumerate(slots):
                here = lanes - (256 // len(groups) * g + member * wide + RS * i)
                at = (here >= 0) & (here < RS)
                val = jnp.where(at, (coords[coord_row, t] * RS + here).astype(F32), val)
        return val[:, 0:128], val[:, 128:256]

    def depth_index(member):
        here = lane - member * 8
        val = zero_row
        for t in range(T):
            at = (here == t) | (here == t + T)
            val = jnp.where(at, coords[2, t].astype(F32), val)
        return val

    loads[0].wait()
    first, second = positions(0, q, SLOTS)
    info_col = jnp.concatenate([first, second, depth_index(q), zero_row], axis=0)
    first, second = positions(1, p, [range(T)])
    info_row = jnp.concatenate([first, second, depth_index(p), zero_row], axis=0)
    for load in loads[3:6]:
        load.wait()
    own = jnp.concatenate([fc[0:4], fc[4:8]], axis=1)
    a_slices, c_own, b_slices = box("a_slices")[0], box("c_own")[0], box("b_slices")[0]
    for j in range(G):
        a_slices[j, 0:4] = fa[4 * j:4 * j + 4]
        a_slices[j, 4:8] = info_col
        c_own[j] = own
        b_slices[j, 0:4] = fb[4 * j:4 * j + 4]
        b_slices[j, 4:8] = info_row

    pl.semaphore_wait(barrier, 2 * (G - 1))
    send("a_slices")
    send("b_slices")
    send("c_own")

    def across_of(info):
        return jnp.concatenate([info[4:5], info[5:6]], axis=1).astype(jnp.int32)

    lane64 = iota((128, 192), 1) % 64

    def back_matrix(info, dst):
        turned = jnp.transpose(info).astype(jnp.int32)
        for half in range(2):
            here = turned[:, 4 + half:5 + half]
            dst[128 * half:128 * half + 128] = (lane64 == here).astype(BF16)
        return turned

    def names_of(name):
        return [name + str(i) for i in range(PARTS)]

    def serve_blocks(w, v, names):
        parts = split(v, 3, 0)
        size = 256 // len(names)
        for i, name in enumerate(names):
            total = mm(w[size * i:size * i + size], parts)
            box(name)[0][...] = total.reshape(G, -1, 128)
            send(name)

    def serve(same, rows, names):
        high, mid, low = split(rows, 3, None)
        most = jnp.concatenate([high, mid], axis=1)
        size = 256 // len(names)
        for i, name in enumerate(names):
            w = same[size * i:size * i + size]
            both = mm(w, most)
            total = both[:, 0:128] + (both[:, 128:256] + mm(w, low))
            box(name)[0][...] = total.reshape(G, -1, 128)
            send(name)

    def rows_of(names):
        boxes = [arrived(name) for name in names]
        return jnp.concatenate([ref[...].reshape(-1, 128) for ref in boxes], axis=0)

    def stacked(src):
        for j in range(G):
            xc[4 * j:4 * j + 4] = src[j]
        return xc[...]

    src = arrived("b_slices")
    info_row = jnp.sum(src[...], axis=0)
    turned_row = back_matrix(info_row, wbt)
    for j in range(G):
        vb[4 * j:4 * j + 4] = src[j, 0:4]
    serve_blocks(wbt, vb[...], ["b_slots"])
    columns_here = split(stacked(arrived("c_own")), 3, 0)
    src = arrived("a_slices")
    info_col = jnp.sum(src[...], axis=0)
    turned_col = back_matrix(info_col, wat)
    k_there = turned_col[:, 6:7]
    down, lane64 = iota((128, 192), 0), iota((128, 192), 1) % 64
    column = (lane64 // 4) * 128 + q * 8 + lane64 % 4
    wanted = jnp.where(down % 8 < T, k_there, -1)
    pick = jnp.concatenate(
        [(wanted == column).astype(BF16), (wanted == column + 4).astype(BF16)], axis=0
    )
    both = mm(pick, columns_here)
    c_out = box("c_slots")[0]
    c_out[...] = (pltpu.roll(both[:128], 64, 1) + both[128:]).reshape(G, 8, 128)[:, 0:4]
    send("c_slots")
    for j in range(G):
        va[4 * j:4 * j + 4] = src[j, 0:4]
    serve_blocks(wat, va[...], names_of("a_slots"))

    for info, turn, w, same in (
        (info_col, turned_col, wa, same_a), (info_row, turned_row, wb, same_b)
    ):
        across = across_of(info)
        w[...] = (iota((64, 256), 0) == across).astype(BF16)
        for half in range(2):
            here = turn[:, 4 + half:5 + half]
            same[128 * half:128 * half + 128] = (
                jnp.broadcast_to(across, (128, 256)) == here
            ).astype(BF16)

    spread = (iota((128, 192), 0) == (lane64 // 4) * 8 + lane64 % 4).astype(BF16)
    k_tiles = jnp.broadcast_to(info_row[6:7], (8, 128))
    k_lane = mm(split(k_tiles, 3, 1), jnp.concatenate([spread, spread, spread], axis=0))
    k_lane = jnp.broadcast_to(k_lane[0:1].astype(jnp.int32), (128, 192))
    mix[0:128] = (k_lane == p * 128 + down).astype(BF16)
    mix[128:256] = (k_lane == wanted).astype(BF16)

    def unpack(src, dst, slots):
        for i, t in enumerate(slots):
            for j in range(G):
                dst[t, 4 * j:4 * j + 4] = src[j, 4 * i:4 * i + 4]

    def pack(i, value, dst):
        for j in range(G):
            dst[j, 4 * i:4 * i + 4] = value[4 * j:4 * j + 4]

    def turned_of(rows):
        return jnp.transpose(jnp.concatenate([rows, jnp.zeros((4, 128), F32)], axis=0))

    def columns(turned):
        return [jnp.broadcast_to(turned[64:128, t:t + 1], (64, 128)) for t in range(T)]

    src = arrived("b_slots")
    unpack(src, tb, range(T))
    for t in range(T):
        tb3[t] = left_of(tb[t])
    src = arrived("c_slots")
    depth = columns(turned_of(jnp.sum(src[...], axis=0)))
    for t in range(T):
        bct3[t] = left_of(jnp.transpose(tb[t] * depth[t]))
    for load in (loads[1], loads[2], loads[6]):
        load.wait()
    for t in range(T):
        datat[t] = jnp.transpose(data[t].astype(F32))

    def norm(value):
        return jnp.sum(value, axis=(0, 1), keepdims=True)

    def live(t):
        return (t < counts[0]).astype(F32)

    def gradients(values_of, name, scalars_of):
        gc_out, gb_out = box(name + "c_in")[0], box(name + "b_in")[0]
        cols = jnp.zeros((64, 128), F32)
        lanes = iota((64, 128), 1)
        for number, slots in enumerate(SLOTS):
            parts = [split(values, 2, None) for values in values_of(number, slots)]
            ga_name = name + "a_in" + str(number)
            for i, t in enumerate(slots):
                high, low = parts[i]
                raw = mm(tb3[t], jnp.concatenate([high, low, high], axis=0))
                pack(i, raw * depth[t], box(ga_name)[0])
                col = jnp.sum(ta[t] * raw, axis=1, keepdims=True)
                cols = jnp.where(lanes == t, col, cols)
            send(ga_name)
            if slots[-1] == T - 1:
                tile = jnp.transpose(jnp.concatenate([cols, jnp.zeros((64, 128), F32)], axis=0))[:4]
                row4, lane4 = iota((4, 128), 0), iota((4, 128), 1)
                for i, scalar in enumerate(scalars_of()):
                    tile = jnp.where((row4 == i) & (lane4 >= 64), scalar, tile)
                for j in range(G):
                    gc_out[j] = tile
                send(name + "c_in")
            for i, t in enumerate(slots):
                high, low = parts[i]
                pack(t, mm(tac3[t], jnp.concatenate([high, low, high], axis=1), 1), gb_out)
        send(name + "b_in")
        return cols

    def data_left(number, slots):
        src = arrived("a_slots" + str(number))
        unpack(src, ta, slots)
        values = []
        for t in slots:
            a3[t] = right_of(ta[t], 0)
            tac3[t] = left_of(ta[t] * depth[t])
            values.append((datat[t] - mm(bct3[t], a3[t])) * live(t))
        return values

    cols_g = gradients(data_left, "g", lambda: ())
    for t in range(T):
        for part in range(3):
            left[t, :, 128 * part:128 * part + 64] = bct3[t, :, 64 * part:64 * part + 64]

    def fold(w, rows, v):
        high, mid, low = split(rows, 3, None)
        most = mm(w[...], jnp.concatenate([high, mid], axis=1))
        v[...] = most[:, 0:128] + (most[:, 128:256] + mm(w[...], low))

    def blend(src):
        both = mm(mix[...], split(stacked(src), 3, 0))
        return jnp.where(iota((128, 128), 1) < 64, both[:128], pltpu.roll(both[128:], 64, 1))

    lane_col = iota((1, 1, 128), 2)

    def send_sums(name, u, base, scalars):
        own = pltpu.roll(u, 64, 1).reshape(G, 8, 128)
        u = u.reshape(G, 8, 128)
        c_put[:, base:base + 4] = jnp.where(lane_col < 64, u[:, 0:4], own[:, 4:8])
        now = u[:, 0:4]
        for i, scalar in enumerate(scalars):
            at = (iota((1, 4, 128), 1) == i) & (iota((1, 4, 128), 2) < 64)
            now = jnp.where(at, jnp.broadcast_to(scalar.reshape(1, 1, 1), (1, 4, 128)), now)
        box(name + "c_out")[0][...] = now
        send(name + "c_out")

    c_put = box("c_put")[0]

    src = arrived("gc_in")
    send_sums("g", blend(src), 0, ())
    rows_b = rows_of(["gb_in"])
    serve(same_b, rows_b, ["gb_out"])
    rows_a = rows_of(names_of("ga_in"))
    serve(same_a, rows_a, names_of("ga_out"))
    fold(wb, rows_b, gb)
    fold(wa, rows_a, ga)
    g_part = norm(ga[...] * ga[...] + gb[...] * gb[...])

    def direction_bc(name):
        src = arrived(name + "b_out")
        unpack(src, db, range(T))
        src = arrived(name + "c_out")
        total = jnp.sum(src[...], axis=0)
        turned = turned_of(total)
        du = columns(turned)
        for t in range(T):
            high, low = split(jnp.transpose(db[t] * depth[t] + tb[t] * du[t]), 2, None)
            left[t, :, 64:128] = high
            left[t, :, 192:256] = high
            left[t, :, 320:384] = low
        return total, turned[64:128]

    def direction_a(name, number, slots):
        src = arrived(name + "a_out" + str(number))
        unpack(src, da, slots)
        products = []
        for t in slots:
            high, low = split(da[t], 2, None)
            right = [high, a3[t, 0:64], low, a3[t, 64:128], high, a3[t, 0:64]]
            products.append(mm(left[t], jnp.concatenate(right, axis=0)) * live(t))
        return products

    _, dirs_g = direction_bc("g")
    g_part = g_part + norm(cols_g[:, 0:8] * dirs_g)

    def second_values(number, slots):
        products = direction_a("g", number, slots)
        for t, product in zip(slots, products):
            jg[t] = product
        return products

    def first_scalars():
        squares = jnp.zeros((128, 128), F32)
        for t in range(T):
            squares = squares + jg[t] * jg[t]
        return g_part, norm(squares)

    cols_w = gradients(second_values, "w", first_scalars)

    src = arrived("wc_in")
    group = jnp.sum(src[...], axis=0)
    send_sums("w", blend(src), 4, (group[0:1, 127:128], group[1:2, 127:128]))
    rows_b = rows_of(["wb_in"])
    serve(same_b, rows_b, ["wb_out"])
    rows_a = rows_of(names_of("wa_in"))
    serve(same_a, rows_a, names_of("wa_out"))
    fold(wb, rows_b, vb)
    fold(wa, rows_a, va)
    total_w, dirs_w = direction_bc("w")
    lam = damp[0]
    g_norm = total_w[0:1, 0:1]
    j_norm = total_w[1:2, 0:1]
    alpha0 = g_norm / (j_norm + lam * g_norm)

    def residual_of(g, w):
        return g - alpha0 * (w + lam * g)

    r_a = residual_of(ga[...], va[...])
    r_b = residual_of(gb[...], vb[...])
    r_cols = residual_of(cols_g[:, 0:8], cols_w[:, 0:8])
    rr_part = norm(r_a * r_a + r_b * r_b) + norm(r_cols * residual_of(dirs_g, dirs_w))
    rg_part = norm(r_a * ga[...] + r_b * gb[...]) + norm(r_cols * dirs_g)
    square = jnp.zeros((128, 128), F32)
    cross = jnp.zeros((128, 128), F32)
    for number, slots in enumerate(SLOTS):
        for t, product in zip(slots, direction_a("w", number, slots)):
            jr = residual_of(jg[t], product)
            square = square + jr * jr
            cross = cross + jr * jg[t]

    parts = (rr_part, rg_part, norm(square), norm(cross))
    row = zero_row
    for i, part in enumerate(parts):
        row = jnp.where(lane // 32 == i, part, row)
    out = box("sum_col")[0]
    for j in range(G):
        out[j] = row
    send("sum_col")
    a_put, b_put = box("a_put")[0], box("b_put")[0]
    for j in range(G):
        a_put[j, 0:4] = ga[4 * j:4 * j + 4]
        a_put[j, 4:8] = va[4 * j:4 * j + 4]
        b_put[j, 0:4] = gb[4 * j:4 * j + 4]
        b_put[j, 4:8] = vb[4 * j:4 * j + 4]
    send("a_put")
    send("b_put")
    send("c_put")

    src = arrived("sum_col")
    row = jnp.sum(src[...], axis=0)
    out = box("sum_row")[0]
    for j in range(G):
        out[j] = row
    send("sum_row")
    src_a = arrived("a_put")
    src_b = arrived("b_put")
    own = jnp.sum(arrived("c_put")[...], axis=0)
    own_g = jnp.concatenate([own[0:4, 0:64], own[0:4, 64:128]], axis=0)
    own_w = jnp.concatenate([own[4:8, 0:64], own[4:8, 64:128]], axis=0)
    for j in range(G):
        ga[4 * j:4 * j + 4] = src_a[j, 0:4]
        va[4 * j:4 * j + 4] = src_a[j, 4:8]
        gb[4 * j:4 * j + 4] = src_b[j, 0:4]
        vb[4 * j:4 * j + 4] = src_b[j, 4:8]
    blocks = ((ga[...], va[...], out_a), (gb[...], vb[...], out_b), (own_g, own_w, out_c))
    bases = [(alpha0 * g, residual_of(g, w), g, out) for g, w, out in blocks]
    src = arrived("sum_row")
    row = jnp.sum(src[...], axis=0)
    r_norm, r_g, jr_norm, jr_jg = [row[:, 32 * i:32 * i + 1] for i in range(4)]
    beta = r_norm / g_norm
    curve = (
        jr_norm + lam * r_norm
        + 2.0 * beta * (jr_jg + lam * r_g)
        + beta * beta * (j_norm + lam * g_norm)
    )
    alpha1 = r_norm / curve

    for base, r, g, out in bases:
        out[...] = base + alpha1 * (r + beta * g)
    for i in range(n):
        wait(send_sem.at[i], outbox[i])


def put(a, b, c, x, y, z):
    x[...] = a[...]
    y[...] = b[...]
    z[...] = c[...]


def per_device(
    tile_data, tile_coords, tile_counts, factor_rows, factor_cols, factor_depth, damping
):
    vmem = pl.BlockSpec(memory_space=pltpu.VMEM)
    boxes = [pltpu.VMEM((G, rows, 128), F32) for _, _, rows in EXCHANGES]
    blocks = ((64, 128), (64, 128), (8, 64))
    steps = pl.pallas_call(
        kernel,
        out_shape=tuple(pltpu.VMEM(block, F32) for block in blocks),
        in_specs=[pl.BlockSpec(memory_space=pltpu.HBM)] * 7,
        out_specs=(vmem, vmem, vmem),
        scratch_shapes=[
            *boxes, *boxes,
            pltpu.SMEM((3, T), jnp.int32), pltpu.SMEM((1,), jnp.int32), pltpu.SMEM((1,), F32),
            pltpu.VMEM((64, 128), F32), pltpu.VMEM((64, 128), F32), pltpu.VMEM((8, 64), F32),
            pltpu.VMEM((T, 128, 128), BF16),
            *[pltpu.VMEM((64, 128), F32)] * 4,
            *[pltpu.VMEM((T, 64, 128), F32)] * 4,
            pltpu.VMEM((T, 128, 128), F32),
            pltpu.VMEM((T, 128, 192), BF16),
            pltpu.VMEM((T, 64, 384), BF16), pltpu.VMEM((T, 64, 384), BF16),
            pltpu.VMEM((T, 192, 128), BF16),
            pltpu.VMEM((T, 128, 384), BF16),
            pltpu.VMEM((T, 128, 128), F32),
            pltpu.VMEM((64, 128), F32),
            pltpu.VMEM((64, 256), BF16), pltpu.VMEM((64, 256), BF16),
            pltpu.VMEM((256, 192), BF16), pltpu.VMEM((256, 192), BF16),
            pltpu.VMEM((256, 256), BF16), pltpu.VMEM((256, 256), BF16),
            pltpu.VMEM((256, 192), BF16),
            pltpu.SemaphoreType.DMA((7,)),
            pltpu.SemaphoreType.DMA((len(EXCHANGES),)),
            pltpu.SemaphoreType.DMA((len(EXCHANGES),)),
        ],
        compiler_params=pltpu.CompilerParams(collective_id=0, has_side_effects=True),
        name="gauss_newton",
    )(
        tile_coords, tile_counts, damping.reshape(1),
        factor_rows, factor_cols, factor_depth.T, tile_data,
    )
    step_a, step_b, step_c = pl.pallas_call(
        put,
        out_shape=tuple(jax.ShapeDtypeStruct(block, F32) for block in blocks),
        in_specs=[vmem, vmem, vmem],
        out_specs=(vmem, vmem, vmem),
        name="put",
    )(*[pltpu.with_memory_space_constraint(step, pltpu.VMEM) for step in steps])
    return step_a, step_b, step_c.T


def solution(mesh):
    both = ("row", "col")
    flip = ("col", "row")
    return jax.shard_map(
        per_device,
        mesh=mesh,
        in_specs=(
            P(both, None, None), P(None, both), P(both),
            P(None, both), P(None, flip), P(None, both), P(),
        ),
        out_specs=(P(None, both), P(None, flip), P(None, both)),
        check_vma=False,
    )
```

```python
import jax
import jax.numpy as jnp
from jax import lax
from jax.experimental import pallas as pl
from jax.experimental.pallas import tpu as pltpu
from jax.sharding import PartitionSpec as P

G = 16
T = 4
RS = 4
F32 = jnp.float32
BF16 = jnp.bfloat16

def ring(d, size):
    return min(d, size - d)


COL_PEERS = sorted(
    [(dz, dc) for dz in range(8) for dc in range(2) if (dz, dc) != (0, 0)],
    key=lambda d: (-(ring(d[0], 8) + d[1]) if d[0] else 0, -d[1], d[0]),
)
ROW_PEERS = sorted(
    [(dy, dx) for dy in range(4) for dx in range(4) if (dy, dx) != (0, 0)],
    key=lambda d: (-(ring(d[0], 4) + ring(d[1], 4)), -ring(d[0], 4)),
)

PARTS = 1
SLOTS = [tuple(range(T // PARTS * i, T // PARTS * (i + 1))) for i in range(PARTS)]


def slot_boxes(name):
    return [(name + str(i), 0, 16 // PARTS) for i in range(PARTS)]


EXCHANGES = (
    ("a_slices", 0, 8), ("c_own", 1, 4), ("b_slices", 1, 8),
    *slot_boxes("a_slots"), ("b_slots", 1, 16), ("c_slots", 0, 2),
    *slot_boxes("ga_in"), ("gc_in", 1, 4), ("gb_in", 1, 16),
    *slot_boxes("ga_out"), ("gb_out", 1, 16), ("gc_out", 0, 2),
    *slot_boxes("wa_in"), ("wc_in", 1, 4), ("wb_in", 1, 16),
    *slot_boxes("wa_out"), ("wb_out", 1, 16), ("wc_out", 0, 4),
    ("a_put", 0, 8), ("b_put", 1, 8), ("c_put", 0, 8),
    ("sum_col", 0, 1), ("sum_row", 1, 1),
)
INDEX = {name: i for i, (name, _, _) in enumerate(EXCHANGES)}


def mm(a, b, rhs_dim=0):
    return lax.dot_general(a, b, (((1,), (rhs_dim,)), ((), ())), preferred_element_type=F32)


def split(x, count, axis):
    parts = []
    for _ in range(count):
        part = x.astype(BF16)
        parts.append(part)
        x = x - part.astype(F32)
    return parts if axis is None else jnp.concatenate(parts, axis=axis)


def left_of(x, axis=1):
    high, low = split(x, 2, None)
    return jnp.concatenate([high, high, low], axis=axis)


def right_of(x, axis):
    high, low = split(x, 2, None)
    return jnp.concatenate([high, low, high], axis=axis)


def iota(shape, dim):
    return lax.broadcasted_iota(jnp.int32, shape, dim)


def kernel(coords_hbm, counts_hbm, damp_hbm, fa_hbm, fb_hbm, fc_hbm, data_hbm, *refs):
    out_a, out_b, out_c = refs[:3]
    refs = refs[3:]
    n = len(EXCHANGES)
    outbox, inbox = refs[:n], refs[n:2 * n]
    (
        coords, counts, damp, fa, fb, fc, data,
        va, vb, ga, gb, ta, tb, da, db, jg,
        bct3, tb3, tac3, a3, left, datat, xc,
        wa, wb, wat, wbt, same_a, same_b, mix, load_sem, send_sem, recv_sem,
    ) = refs[2 * n:]
    p = lax.axis_index("row")
    q = lax.axis_index("col")
    z, core = q // 2, q % 2
    col_of = [((z + dz) % 8) * 2 + (core + dc) % 2 for dz, dc in COL_PEERS]
    y, x = p // 4, p % 4
    row_of = [((y + dy) % 4) * 4 + (x + dx) % 4 for dy, dx in ROW_PEERS]

    barrier = pltpu.get_barrier_semaphore()
    for peer in col_of:
        pl.semaphore_signal(barrier, inc=1, device_id={"col": peer})
    for peer in row_of:
        pl.semaphore_signal(barrier, inc=1, device_id={"row": peer})

    loads = [
        pltpu.make_async_copy(src, dst, load_sem.at[i])
        for i, (src, dst) in enumerate((
            (coords_hbm, coords), (counts_hbm, counts), (damp_hbm, damp),
            (fa_hbm, fa), (fb_hbm, fb), (fc_hbm, fc), (data_hbm, data),
        ))
    ]
    for load in loads:
        load.start()

    def box(name):
        return outbox[INDEX[name]], inbox[INDEX[name]]

    def send(name):
        i = INDEX[name]
        me, peers, axis = ((q, col_of, "col"), (p, row_of, "row"))[EXCHANGES[i][1]]
        src, dst = outbox[i], inbox[i]
        for peer in peers:
            pltpu.make_async_remote_copy(
                src_ref=src.at[peer],
                dst_ref=dst.at[me],
                send_sem=send_sem.at[i],
                recv_sem=recv_sem.at[i],
                device_id={axis: peer},
            ).start()
        dst[me] = src[me]

    def wait(sem, ref):
        some = ref.at[pl.ds(0, G - 1)]
        pltpu.make_async_copy(some, some, sem).wait()

    def arrived(name):
        i = INDEX[name]
        wait(recv_sem.at[i], inbox[i])
        return inbox[i]

    lane = iota((1, 128), 1)
    zero_row = jnp.zeros((1, 128), F32)

    def positions(coord_row, member, groups):
        wide = 16 // len(groups)
        lanes = iota((1, 256), 1)
        val = jnp.zeros((1, 256), F32)
        for g, slots in enumerate(groups):
            for i, t in enumerate(slots):
                here = lanes - (256 // len(groups) * g + member * wide + RS * i)
                at = (here >= 0) & (here < RS)
                val = jnp.where(at, (coords[coord_row, t] * RS + here).astype(F32), val)
        return val[:, 0:128], val[:, 128:256]

    def depth_index(member):
        here = lane - member * 8
        val = zero_row
        for t in range(T):
            at = (here == t) | (here == t + T)
            val = jnp.where(at, coords[2, t].astype(F32), val)
        return val

    loads[0].wait()
    first, second = positions(0, q, SLOTS)
    info_col = jnp.concatenate([first, second, depth_index(q), zero_row], axis=0)
    first, second = positions(1, p, [range(T)])
    info_row = jnp.concatenate([first, second, depth_index(p), zero_row], axis=0)
    for load in loads[3:6]:
        load.wait()
    own = jnp.concatenate([fc[0:4], fc[4:8]], axis=1)
    a_slices, c_own, b_slices = box("a_slices")[0], box("c_own")[0], box("b_slices")[0]
    for j in range(G):
        a_slices[j, 0:4] = fa[4 * j:4 * j + 4]
        a_slices[j, 4:8] = info_col
        c_own[j] = own
        b_slices[j, 0:4] = fb[4 * j:4 * j + 4]
        b_slices[j, 4:8] = info_row

    pl.semaphore_wait(barrier, 2 * (G - 1))
    send("a_slices")
    send("b_slices")
    send("c_own")

    def across_of(info):
        return jnp.concatenate([info[4:5], info[5:6]], axis=1).astype(jnp.int32)

    lane64 = iota((128, 192), 1) % 64

    def back_matrix(info, dst):
        turned = jnp.transpose(info).astype(jnp.int32)
        for half in range(2):
            here = turned[:, 4 + half:5 + half]
            dst[128 * half:128 * half + 128] = (lane64 == here).astype(BF16)
        return turned

    def names_of(name):
        return [name + str(i) for i in range(PARTS)]

    def serve_blocks(w, v, names):
        parts = split(v, 3, 0)
        size = 256 // len(names)
        for i, name in enumerate(names):
            total = mm(w[size * i:size * i + size], parts)
            box(name)[0][...] = total.reshape(G, -1, 128)
            send(name)

    def serve(same, rows, names):
        high, mid, low = split(rows, 3, None)
        most = jnp.concatenate([high, mid], axis=1)
        size = 256 // len(names)
        for i, name in enumerate(names):
            w = same[size * i:size * i + size]
            both = mm(w, most)
            total = both[:, 0:128] + (both[:, 128:256] + mm(w, low))
            box(name)[0][...] = total.reshape(G, -1, 128)
            send(name)

    def rows_of(names):
        boxes = [arrived(name) for name in names]
        return jnp.concatenate([ref[...].reshape(-1, 128) for ref in boxes], axis=0)

    def folded(u):
        turned = pltpu.roll(u, 64, 1).reshape(G, 8, 128)
        return jnp.where(iota((1, 1, 128), 2) < 64, turned[:, 0:2], u.reshape(G, 8, 128)[:, 2:4])

    def unfolded(rows):
        return jnp.concatenate([pltpu.roll(rows, 64, 1), rows], axis=0)

    def stacked(src):
        for j in range(G):
            xc[4 * j:4 * j + 4] = src[j]
        return xc[...]

    src = arrived("b_slices")
    info_row = jnp.sum(src[...], axis=0)
    turned_row = back_matrix(info_row, wbt)
    for j in range(G):
        vb[4 * j:4 * j + 4] = src[j, 0:4]
    serve_blocks(wbt, vb[...], ["b_slots"])
    columns_here = split(stacked(arrived("c_own")), 3, 0)
    src = arrived("a_slices")
    info_col = jnp.sum(src[...], axis=0)
    turned_col = back_matrix(info_col, wat)
    k_there = turned_col[:, 6:7]
    down, lane64 = iota((128, 192), 0), iota((128, 192), 1) % 64
    column = (lane64 // 4) * 128 + q * 8 + lane64 % 4
    wanted = jnp.where(down % 8 < T, k_there, -1)
    pick = jnp.concatenate(
        [(wanted == column).astype(BF16), (wanted == column + 4).astype(BF16)], axis=0
    )
    both = mm(pick, columns_here)
    c_out = box("c_slots")[0]
    c_out[...] = folded(pltpu.roll(both[:128], 64, 1) + both[128:])
    send("c_slots")
    for j in range(G):
        va[4 * j:4 * j + 4] = src[j, 0:4]
    serve_blocks(wat, va[...], names_of("a_slots"))

    for info, turn, w, same in (
        (info_col, turned_col, wa, same_a), (info_row, turned_row, wb, same_b)
    ):
        across = across_of(info)
        w[...] = (iota((64, 256), 0) == across).astype(BF16)
        for half in range(2):
            here = turn[:, 4 + half:5 + half]
            same[128 * half:128 * half + 128] = (
                jnp.broadcast_to(across, (128, 256)) == here
            ).astype(BF16)

    spread = (iota((128, 192), 0) == (lane64 // 4) * 8 + lane64 % 4).astype(BF16)
    k_tiles = jnp.broadcast_to(info_row[6:7], (8, 128))
    k_lane = mm(split(k_tiles, 3, 1), jnp.concatenate([spread, spread, spread], axis=0))
    k_lane = jnp.broadcast_to(k_lane[0:1].astype(jnp.int32), (128, 192))
    mix[0:128] = (k_lane == p * 128 + down).astype(BF16)
    mix[128:256] = (k_lane == wanted).astype(BF16)

    def unpack(src, dst, slots):
        for i, t in enumerate(slots):
            for j in range(G):
                dst[t, 4 * j:4 * j + 4] = src[j, 4 * i:4 * i + 4]

    def pack(i, value, dst):
        for j in range(G):
            dst[j, 4 * i:4 * i + 4] = value[4 * j:4 * j + 4]

    def turned_of(rows):
        return jnp.transpose(jnp.concatenate([rows, jnp.zeros((4, 128), F32)], axis=0))

    def columns(turned):
        return [jnp.broadcast_to(turned[64:128, t:t + 1], (64, 128)) for t in range(T)]

    src = arrived("b_slots")
    unpack(src, tb, range(T))
    for t in range(T):
        tb3[t] = left_of(tb[t])
    src = arrived("c_slots")
    depth = columns(turned_of(unfolded(jnp.sum(src[...], axis=0))))
    for t in range(T):
        bct3[t] = left_of(jnp.transpose(tb[t] * depth[t]))
    for load in (loads[1], loads[2], loads[6]):
        load.wait()
    for t in range(T):
        datat[t] = jnp.transpose(data[t].astype(F32))

    def norm(value):
        return jnp.sum(value, axis=(0, 1), keepdims=True)

    def live(t):
        return (t < counts[0]).astype(F32)

    def gradients(values_of, name, scalars_of):
        gc_out, gb_out = box(name + "c_in")[0], box(name + "b_in")[0]
        cols = jnp.zeros((64, 128), F32)
        lanes = iota((64, 128), 1)
        for number, slots in enumerate(SLOTS):
            parts = [split(values, 2, None) for values in values_of(number, slots)]
            ga_name = name + "a_in" + str(number)
            for i, t in enumerate(slots):
                high, low = parts[i]
                raw = mm(tb3[t], jnp.concatenate([high, low, high], axis=0))
                pack(i, raw * depth[t], box(ga_name)[0])
                col = jnp.sum(ta[t] * raw, axis=1, keepdims=True)
                cols = jnp.where(lanes == t, col, cols)
            send(ga_name)
            if slots[-1] == T - 1:
                tile = jnp.transpose(jnp.concatenate([cols, jnp.zeros((64, 128), F32)], axis=0))[:4]
                row4, lane4 = iota((4, 128), 0), iota((4, 128), 1)
                for i, scalar in enumerate(scalars_of()):
                    tile = jnp.where((row4 == i) & (lane4 >= 64), scalar, tile)
                for j in range(G):
                    gc_out[j] = tile
                send(name + "c_in")
            for i, t in enumerate(slots):
                high, low = parts[i]
                pack(t, mm(tac3[t], jnp.concatenate([high, low, high], axis=1), 1), gb_out)
        send(name + "b_in")
        return cols

    def data_left(number, slots):
        src = arrived("a_slots" + str(number))
        unpack(src, ta, slots)
        values = []
        for t in slots:
            a3[t] = right_of(ta[t], 0)
            tac3[t] = left_of(ta[t] * depth[t])
            values.append((datat[t] - mm(bct3[t], a3[t])) * live(t))
        return values

    cols_g = gradients(data_left, "g", lambda: ())
    for t in range(T):
        for part in range(3):
            left[t, :, 128 * part:128 * part + 64] = bct3[t, :, 64 * part:64 * part + 64]

    def fold(w, rows, v):
        high, mid, low = split(rows, 3, None)
        most = mm(w[...], jnp.concatenate([high, mid], axis=1))
        v[...] = most[:, 0:128] + (most[:, 128:256] + mm(w[...], low))

    def blend(src):
        both = mm(mix[...], split(stacked(src), 3, 0))
        return jnp.where(iota((128, 128), 1) < 64, both[:128], pltpu.roll(both[128:], 64, 1))

    lane_col = iota((1, 1, 128), 2)

    def send_sums(name, u, base, scalars):
        own = pltpu.roll(u, 64, 1).reshape(G, 8, 128)
        now = folded(u)
        u = u.reshape(G, 8, 128)
        c_put[:, base:base + 4] = jnp.where(lane_col < 64, u[:, 0:4], own[:, 4:8])
        if scalars:
            now = u[:, 0:4]
        for i, scalar in enumerate(scalars):
            at = (iota((1, 4, 128), 1) == i) & (iota((1, 4, 128), 2) < 64)
            now = jnp.where(at, jnp.broadcast_to(scalar.reshape(1, 1, 1), (1, 4, 128)), now)
        box(name + "c_out")[0][...] = now
        send(name + "c_out")

    c_put = box("c_put")[0]

    src = arrived("gc_in")
    send_sums("g", blend(src), 0, ())
    rows_b = rows_of(["gb_in"])
    serve(same_b, rows_b, ["gb_out"])
    rows_a = rows_of(names_of("ga_in"))
    serve(same_a, rows_a, names_of("ga_out"))
    fold(wb, rows_b, gb)
    fold(wa, rows_a, ga)
    g_part = norm(ga[...] * ga[...] + gb[...] * gb[...])

    def direction_bc(name):
        src = arrived(name + "b_out")
        unpack(src, db, range(T))
        src = arrived(name + "c_out")
        total = jnp.sum(src[...], axis=0)
        turned = turned_of(total if total.shape[0] == 4 else unfolded(total))
        du = columns(turned)
        for t in range(T):
            high, low = split(jnp.transpose(db[t] * depth[t] + tb[t] * du[t]), 2, None)
            left[t, :, 64:128] = high
            left[t, :, 192:256] = high
            left[t, :, 320:384] = low
        return total, turned[64:128]

    def direction_a(name, number, slots):
        src = arrived(name + "a_out" + str(number))
        unpack(src, da, slots)
        products = []
        for t in slots:
            high, low = split(da[t], 2, None)
            right = [high, a3[t, 0:64], low, a3[t, 64:128], high, a3[t, 0:64]]
            products.append(mm(left[t], jnp.concatenate(right, axis=0)) * live(t))
        return products

    _, dirs_g = direction_bc("g")
    g_part = g_part + norm(cols_g[:, 0:8] * dirs_g)

    def second_values(number, slots):
        products = direction_a("g", number, slots)
        for t, product in zip(slots, products):
            jg[t] = product
        return products

    def first_scalars():
        squares = jnp.zeros((128, 128), F32)
        for t in range(T):
            squares = squares + jg[t] * jg[t]
        return g_part, norm(squares)

    cols_w = gradients(second_values, "w", first_scalars)

    src = arrived("wc_in")
    group = jnp.sum(src[...], axis=0)
    send_sums("w", blend(src), 4, (group[0:1, 127:128], group[1:2, 127:128]))
    rows_b = rows_of(["wb_in"])
    serve(same_b, rows_b, ["wb_out"])
    rows_a = rows_of(names_of("wa_in"))
    serve(same_a, rows_a, names_of("wa_out"))
    fold(wb, rows_b, vb)
    fold(wa, rows_a, va)
    total_w, dirs_w = direction_bc("w")
    lam = damp[0]
    g_norm = total_w[0:1, 0:1]
    j_norm = total_w[1:2, 0:1]
    alpha0 = g_norm / (j_norm + lam * g_norm)

    def residual_of(g, w):
        return g - alpha0 * (w + lam * g)

    r_a = residual_of(ga[...], va[...])
    r_b = residual_of(gb[...], vb[...])
    r_cols = residual_of(cols_g[:, 0:8], cols_w[:, 0:8])
    rr_part = norm(r_a * r_a + r_b * r_b) + norm(r_cols * residual_of(dirs_g, dirs_w))
    rg_part = norm(r_a * ga[...] + r_b * gb[...]) + norm(r_cols * dirs_g)
    square = jnp.zeros((128, 128), F32)
    cross = jnp.zeros((128, 128), F32)
    for number, slots in enumerate(SLOTS):
        for t, product in zip(slots, direction_a("w", number, slots)):
            jr = residual_of(jg[t], product)
            square = square + jr * jr
            cross = cross + jr * jg[t]

    parts = (rr_part, rg_part, norm(square), norm(cross))
    row = zero_row
    for i, part in enumerate(parts):
        row = jnp.where(lane // 32 == i, part, row)
    out = box("sum_col")[0]
    for j in range(G):
        out[j] = row
    send("sum_col")
    a_put, b_put = box("a_put")[0], box("b_put")[0]
    for j in range(G):
        a_put[j, 0:4] = ga[4 * j:4 * j + 4]
        a_put[j, 4:8] = va[4 * j:4 * j + 4]
        b_put[j, 0:4] = gb[4 * j:4 * j + 4]
        b_put[j, 4:8] = vb[4 * j:4 * j + 4]
    send("a_put")
    send("b_put")
    send("c_put")

    src = arrived("sum_col")
    row = jnp.sum(src[...], axis=0)
    out = box("sum_row")[0]
    for j in range(G):
        out[j] = row
    send("sum_row")
    src_a = arrived("a_put")
    src_b = arrived("b_put")
    own = jnp.sum(arrived("c_put")[...], axis=0)
    own_g = jnp.concatenate([own[0:4, 0:64], own[0:4, 64:128]], axis=0)
    own_w = jnp.concatenate([own[4:8, 0:64], own[4:8, 64:128]], axis=0)
    for j in range(G):
        ga[4 * j:4 * j + 4] = src_a[j, 0:4]
        va[4 * j:4 * j + 4] = src_a[j, 4:8]
        gb[4 * j:4 * j + 4] = src_b[j, 0:4]
        vb[4 * j:4 * j + 4] = src_b[j, 4:8]
    blocks = ((ga[...], va[...], out_a), (gb[...], vb[...], out_b), (own_g, own_w, out_c))
    bases = [(alpha0 * g, residual_of(g, w), g, out) for g, w, out in blocks]
    src = arrived("sum_row")
    row = jnp.sum(src[...], axis=0)
    r_norm, r_g, jr_norm, jr_jg = [row[:, 32 * i:32 * i + 1] for i in range(4)]
    beta = r_norm / g_norm
    curve = (
        jr_norm + lam * r_norm
        + 2.0 * beta * (jr_jg + lam * r_g)
        + beta * beta * (j_norm + lam * g_norm)
    )
    alpha1 = r_norm / curve

    for base, r, g, out in bases:
        out[...] = base + alpha1 * (r + beta * g)
    for i in range(n):
        wait(send_sem.at[i], outbox[i])


def put(a, b, c, x, y, z):
    x[...] = a[...]
    y[...] = b[...]
    z[...] = c[...]


def per_device(
    tile_data, tile_coords, tile_counts, factor_rows, factor_cols, factor_depth, damping
):
    vmem = pl.BlockSpec(memory_space=pltpu.VMEM)
    boxes = [pltpu.VMEM((G, rows, 128), F32) for _, _, rows in EXCHANGES]
    blocks = ((64, 128), (64, 128), (8, 64))
    steps = pl.pallas_call(
        kernel,
        out_shape=tuple(pltpu.VMEM(block, F32) for block in blocks),
        in_specs=[pl.BlockSpec(memory_space=pltpu.HBM)] * 7,
        out_specs=(vmem, vmem, vmem),
        scratch_shapes=[
            *boxes, *boxes,
            pltpu.SMEM((3, T), jnp.int32), pltpu.SMEM((1,), jnp.int32), pltpu.SMEM((1,), F32),
            pltpu.VMEM((64, 128), F32), pltpu.VMEM((64, 128), F32), pltpu.VMEM((8, 64), F32),
            pltpu.VMEM((T, 128, 128), BF16),
            *[pltpu.VMEM((64, 128), F32)] * 4,
            *[pltpu.VMEM((T, 64, 128), F32)] * 4,
            pltpu.VMEM((T, 128, 128), F32),
            pltpu.VMEM((T, 128, 192), BF16),
            pltpu.VMEM((T, 64, 384), BF16), pltpu.VMEM((T, 64, 384), BF16),
            pltpu.VMEM((T, 192, 128), BF16),
            pltpu.VMEM((T, 128, 384), BF16),
            pltpu.VMEM((T, 128, 128), F32),
            pltpu.VMEM((64, 128), F32),
            pltpu.VMEM((64, 256), BF16), pltpu.VMEM((64, 256), BF16),
            pltpu.VMEM((256, 192), BF16), pltpu.VMEM((256, 192), BF16),
            pltpu.VMEM((256, 256), BF16), pltpu.VMEM((256, 256), BF16),
            pltpu.VMEM((256, 192), BF16),
            pltpu.SemaphoreType.DMA((7,)),
            pltpu.SemaphoreType.DMA((len(EXCHANGES),)),
            pltpu.SemaphoreType.DMA((len(EXCHANGES),)),
        ],
        compiler_params=pltpu.CompilerParams(collective_id=0, has_side_effects=True),
        name="gauss_newton",
    )(
        tile_coords, tile_counts, damping.reshape(1),
        factor_rows, factor_cols, factor_depth.T, tile_data,
    )
    step_a, step_b, step_c = pl.pallas_call(
        put,
        out_shape=tuple(jax.ShapeDtypeStruct(block, F32) for block in blocks),
        in_specs=[vmem, vmem, vmem],
        out_specs=(vmem, vmem, vmem),
        name="put",
    )(*[pltpu.with_memory_space_constraint(step, pltpu.VMEM) for step in steps])
    return step_a, step_b, step_c.T


def solution(mesh):
    both = ("row", "col")
    flip = ("col", "row")
    return jax.shard_map(
        per_device,
        mesh=mesh,
        in_specs=(
            P(both, None, None), P(None, both), P(both),
            P(None, both), P(None, flip), P(None, both), P(),
        ),
        out_specs=(P(None, both), P(None, flip), P(None, both)),
        check_vma=False,
    )
```

```python
import jax
import jax.numpy as jnp
from jax import lax
from jax.experimental import pallas as pl
from jax.experimental.pallas import tpu as pltpu
from jax.sharding import PartitionSpec as P

G = 16
T = 4
RS = 4
F32 = jnp.float32
BF16 = jnp.bfloat16

def ring(d, size):
    return min(d, size - d)


COL_PEERS = sorted(
    [(dz, dc) for dz in range(8) for dc in range(2) if (dz, dc) != (0, 0)],
    key=lambda d: (-(ring(d[0], 8) + d[1]) if d[0] else 0, -d[1], d[0]),
)
ROW_PEERS = sorted(
    [(dy, dx) for dy in range(4) for dx in range(4) if (dy, dx) != (0, 0)],
    key=lambda d: (-(ring(d[0], 4) + ring(d[1], 4)), -ring(d[0], 4)),
)

PARTS = 1
SLOTS = [tuple(range(T // PARTS * i, T // PARTS * (i + 1))) for i in range(PARTS)]


def slot_boxes(name):
    return [(name + str(i), 0, 16 // PARTS) for i in range(PARTS)]


EXCHANGES = (
    ("a_slices", 0, 8), ("c_own", 1, 4), ("b_slices", 1, 8),
    *slot_boxes("a_slots"), ("b_slots", 1, 16), ("c_slots", 0, 2),
    *slot_boxes("ga_in"), ("gc_in", 1, 4), ("gb_in", 1, 16),
    *slot_boxes("ga_out"), ("gb_out", 1, 16), ("gc_out", 0, 2),
    *slot_boxes("wa_in"), ("wc_in", 1, 4), ("wb_in", 1, 16),
    *slot_boxes("wa_out"), ("wb_out", 1, 16), ("wc_out", 0, 4),
    ("a_put", 0, 8), ("b_put", 1, 8), ("c_put", 0, 8),
    ("sum_col", 0, 1), ("sum_row", 1, 1),
)
INDEX = {name: i for i, (name, _, _) in enumerate(EXCHANGES)}

AFTER = {
    "wa_in0": "ga_in0", "wb_in": "gb_in", "wc_in": "gc_in", "wa_out0": "ga_out0", "wb_out": "gb_out",
    "a_put": "a_slices", "b_put": "b_slices", "c_put": "c_slots",
    "sum_col": "a_slots0", "sum_row": "c_own",
}
FIRST = [name for name, _, _ in EXCHANGES if name not in AFTER]
SEM = {name: FIRST.index(AFTER.get(name, name)) for name, _, _ in EXCHANGES}


def mm(a, b, rhs_dim=0):
    return lax.dot_general(a, b, (((1,), (rhs_dim,)), ((), ())), preferred_element_type=F32)


def split(x, count, axis):
    parts = []
    for _ in range(count):
        part = x.astype(BF16)
        parts.append(part)
        x = x - part.astype(F32)
    return parts if axis is None else jnp.concatenate(parts, axis=axis)


def left_of(x, axis=1):
    high, low = split(x, 2, None)
    return jnp.concatenate([high, high, low], axis=axis)


def right_of(x, axis):
    high, low = split(x, 2, None)
    return jnp.concatenate([high, low, high], axis=axis)


def iota(shape, dim):
    return lax.broadcasted_iota(jnp.int32, shape, dim)


def kernel(coords_hbm, counts_hbm, damp_hbm, fa_hbm, fb_hbm, fc_hbm, data_hbm, *refs):
    out_a, out_b, out_c = refs[:3]
    refs = refs[3:]
    n = len(EXCHANGES)
    outbox, inbox = refs[:n], refs[n:2 * n]
    (
        coords, counts, damp, fa, fb, fc, data,
        va, vb, ga, gb, ta, tb, da, db, jg,
        bct3, tb3, tac3, a3, left, datat, xc,
        wa, wb, wat, wbt, same_a, same_b, mix, load_sem, send_sem, recv_sem,
    ) = refs[2 * n:]
    p = lax.axis_index("row")
    q = lax.axis_index("col")
    z, core = q // 2, q % 2
    col_of = [((z + dz) % 8) * 2 + (core + dc) % 2 for dz, dc in COL_PEERS]
    y, x = p // 4, p % 4
    row_of = [((y + dy) % 4) * 4 + (x + dx) % 4 for dy, dx in ROW_PEERS]

    barrier = pltpu.get_barrier_semaphore()
    for peer in col_of:
        pl.semaphore_signal(barrier, inc=1, device_id={"col": peer})
    for peer in row_of:
        pl.semaphore_signal(barrier, inc=1, device_id={"row": peer})

    loads = [
        pltpu.make_async_copy(src, dst, load_sem.at[i])
        for i, (src, dst) in enumerate((
            (coords_hbm, coords), (counts_hbm, counts), (damp_hbm, damp),
            (fa_hbm, fa), (fb_hbm, fb), (fc_hbm, fc), (data_hbm, data),
        ))
    ]
    for load in loads:
        load.start()

    def box(name):
        return outbox[INDEX[name]], inbox[INDEX[name]]

    def send(name):
        i = INDEX[name]
        me, peers, axis = ((q, col_of, "col"), (p, row_of, "row"))[EXCHANGES[i][1]]
        src, dst = outbox[i], inbox[i]
        for peer in peers:
            pltpu.make_async_remote_copy(
                src_ref=src.at[peer],
                dst_ref=dst.at[me],
                send_sem=send_sem.at[SEM[name]],
                recv_sem=recv_sem.at[SEM[name]],
                device_id={axis: peer},
            ).start()
        dst[me] = src[me]

    def wait(sem, ref):
        some = ref.at[pl.ds(0, G - 1)]
        pltpu.make_async_copy(some, some, sem).wait()

    def arrived(name):
        i = INDEX[name]
        wait(recv_sem.at[SEM[name]], inbox[i])
        return inbox[i]

    left_over = [name for name, _, _ in EXCHANGES]

    def settle(*names):
        for name in names:
            wait(send_sem.at[SEM[name]], outbox[INDEX[name]])
            left_over.remove(name)

    lane = iota((1, 128), 1)
    zero_row = jnp.zeros((1, 128), F32)

    def positions(coord_row, member, groups):
        wide = 16 // len(groups)
        lanes = iota((1, 256), 1)
        val = jnp.zeros((1, 256), F32)
        for g, slots in enumerate(groups):
            for i, t in enumerate(slots):
                here = lanes - (256 // len(groups) * g + member * wide + RS * i)
                at = (here >= 0) & (here < RS)
                val = jnp.where(at, (coords[coord_row, t] * RS + here).astype(F32), val)
        return val[:, 0:128], val[:, 128:256]

    def depth_index(member):
        here = lane - member * 8
        val = zero_row
        for t in range(T):
            at = (here == t) | (here == t + T)
            val = jnp.where(at, coords[2, t].astype(F32), val)
        return val

    loads[0].wait()
    first, second = positions(0, q, SLOTS)
    info_col = jnp.concatenate([first, second, depth_index(q), zero_row], axis=0)
    first, second = positions(1, p, [range(T)])
    info_row = jnp.concatenate([first, second, depth_index(p), zero_row], axis=0)
    for load in loads[3:6]:
        load.wait()
    own = jnp.concatenate([fc[0:4], fc[4:8]], axis=1)
    a_slices, c_own, b_slices = box("a_slices")[0], box("c_own")[0], box("b_slices")[0]
    for j in range(G):
        a_slices[j, 0:4] = fa[4 * j:4 * j + 4]
        a_slices[j, 4:8] = info_col
        c_own[j] = own
        b_slices[j, 0:4] = fb[4 * j:4 * j + 4]
        b_slices[j, 4:8] = info_row

    pl.semaphore_wait(barrier, 2 * (G - 1))
    send("a_slices")
    send("b_slices")
    send("c_own")

    def across_of(info):
        return jnp.concatenate([info[4:5], info[5:6]], axis=1).astype(jnp.int32)

    lane64 = iota((128, 192), 1) % 64

    def back_matrix(info, dst):
        turned = jnp.transpose(info).astype(jnp.int32)
        for half in range(2):
            here = turned[:, 4 + half:5 + half]
            dst[128 * half:128 * half + 128] = (lane64 == here).astype(BF16)
        return turned

    def names_of(name):
        return [name + str(i) for i in range(PARTS)]

    def serve_blocks(w, v, names):
        parts = split(v, 3, 0)
        size = 256 // len(names)
        for i, name in enumerate(names):
            total = mm(w[size * i:size * i + size], parts)
            box(name)[0][...] = total.reshape(G, -1, 128)
            send(name)

    def serve(same, rows, names):
        high, mid, low = split(rows, 3, None)
        most = jnp.concatenate([high, mid], axis=1)
        size = 256 // len(names)
        for i, name in enumerate(names):
            w = same[size * i:size * i + size]
            both = mm(w, most)
            total = both[:, 0:128] + (both[:, 128:256] + mm(w, low))
            box(name)[0][...] = total.reshape(G, -1, 128)
            send(name)

    def rows_of(names):
        boxes = [arrived(name) for name in names]
        return jnp.concatenate([ref[...].reshape(-1, 128) for ref in boxes], axis=0)

    def folded(u):
        turned = pltpu.roll(u, 64, 1).reshape(G, 8, 128)
        return jnp.where(iota((1, 1, 128), 2) < 64, turned[:, 0:2], u.reshape(G, 8, 128)[:, 2:4])

    def unfolded(rows):
        return jnp.concatenate([pltpu.roll(rows, 64, 1), rows], axis=0)

    def stacked(src):
        for j in range(G):
            xc[4 * j:4 * j + 4] = src[j]
        return xc[...]

    src = arrived("b_slices")
    info_row = jnp.sum(src[...], axis=0)
    turned_row = back_matrix(info_row, wbt)
    for j in range(G):
        vb[4 * j:4 * j + 4] = src[j, 0:4]
    serve_blocks(wbt, vb[...], ["b_slots"])
    columns_here = split(stacked(arrived("c_own")), 3, 0)
    src = arrived("a_slices")
    info_col = jnp.sum(src[...], axis=0)
    turned_col = back_matrix(info_col, wat)
    k_there = turned_col[:, 6:7]
    down, lane64 = iota((128, 192), 0), iota((128, 192), 1) % 64
    column = (lane64 // 4) * 128 + q * 8 + lane64 % 4
    wanted = jnp.where(down % 8 < T, k_there, -1)
    pick = jnp.concatenate(
        [(wanted == column).astype(BF16), (wanted == column + 4).astype(BF16)], axis=0
    )
    both = mm(pick, columns_here)
    c_out = box("c_slots")[0]
    c_out[...] = folded(pltpu.roll(both[:128], 64, 1) + both[128:])
    send("c_slots")
    for j in range(G):
        va[4 * j:4 * j + 4] = src[j, 0:4]
    serve_blocks(wat, va[...], names_of("a_slots"))

    for info, turn, w, same in (
        (info_col, turned_col, wa, same_a), (info_row, turned_row, wb, same_b)
    ):
        across = across_of(info)
        w[...] = (iota((64, 256), 0) == across).astype(BF16)
        for half in range(2):
            here = turn[:, 4 + half:5 + half]
            same[128 * half:128 * half + 128] = (
                jnp.broadcast_to(across, (128, 256)) == here
            ).astype(BF16)

    spread = (iota((128, 192), 0) == (lane64 // 4) * 8 + lane64 % 4).astype(BF16)
    k_tiles = jnp.broadcast_to(info_row[6:7], (8, 128))
    k_lane = mm(split(k_tiles, 3, 1), jnp.concatenate([spread, spread, spread], axis=0))
    k_lane = jnp.broadcast_to(k_lane[0:1].astype(jnp.int32), (128, 192))
    mix[0:128] = (k_lane == p * 128 + down).astype(BF16)
    mix[128:256] = (k_lane == wanted).astype(BF16)

    def unpack(src, dst, slots):
        for i, t in enumerate(slots):
            for j in range(G):
                dst[t, 4 * j:4 * j + 4] = src[j, 4 * i:4 * i + 4]

    def pack(i, value, dst):
        for j in range(G):
            dst[j, 4 * i:4 * i + 4] = value[4 * j:4 * j + 4]

    def turned_of(rows):
        return jnp.transpose(jnp.concatenate([rows, jnp.zeros((4, 128), F32)], axis=0))

    def columns(turned):
        return [jnp.broadcast_to(turned[64:128, t:t + 1], (64, 128)) for t in range(T)]

    src = arrived("b_slots")
    unpack(src, tb, range(T))
    for t in range(T):
        tb3[t] = left_of(tb[t])
    src = arrived("c_slots")
    depth = columns(turned_of(unfolded(jnp.sum(src[...], axis=0))))
    for t in range(T):
        bct3[t] = left_of(jnp.transpose(tb[t] * depth[t]))
    for load in (loads[1], loads[2], loads[6]):
        load.wait()
    for t in range(T):
        datat[t] = jnp.transpose(data[t].astype(F32))

    def norm(value):
        return jnp.sum(value, axis=(0, 1), keepdims=True)

    def live(t):
        return (t < counts[0]).astype(F32)

    def gradients(values_of, name, scalars_of):
        gc_out, gb_out = box(name + "c_in")[0], box(name + "b_in")[0]
        cols = jnp.zeros((64, 128), F32)
        lanes = iota((64, 128), 1)
        for number, slots in enumerate(SLOTS):
            parts = [split(values, 2, None) for values in values_of(number, slots)]
            ga_name = name + "a_in" + str(number)
            for i, t in enumerate(slots):
                high, low = parts[i]
                raw = mm(tb3[t], jnp.concatenate([high, low, high], axis=0))
                pack(i, raw * depth[t], box(ga_name)[0])
                col = jnp.sum(ta[t] * raw, axis=1, keepdims=True)
                cols = jnp.where(lanes == t, col, cols)
            send(ga_name)
            if slots[-1] == T - 1:
                tile = jnp.transpose(jnp.concatenate([cols, jnp.zeros((64, 128), F32)], axis=0))[:4]
                row4, lane4 = iota((4, 128), 0), iota((4, 128), 1)
                for i, scalar in enumerate(scalars_of()):
                    tile = jnp.where((row4 == i) & (lane4 >= 64), scalar, tile)
                for j in range(G):
                    gc_out[j] = tile
                send(name + "c_in")
            for i, t in enumerate(slots):
                high, low = parts[i]
                pack(t, mm(tac3[t], jnp.concatenate([high, low, high], axis=1), 1), gb_out)
        send(name + "b_in")
        return cols

    def data_left(number, slots):
        src = arrived("a_slots" + str(number))
        unpack(src, ta, slots)
        values = []
        for t in slots:
            a3[t] = right_of(ta[t], 0)
            tac3[t] = left_of(ta[t] * depth[t])
            values.append((datat[t] - mm(bct3[t], a3[t])) * live(t))
        return values

    cols_g = gradients(data_left, "g", lambda: ())
    for t in range(T):
        for part in range(3):
            left[t, :, 128 * part:128 * part + 64] = bct3[t, :, 64 * part:64 * part + 64]

    def fold(w, rows, v):
        high, mid, low = split(rows, 3, None)
        most = mm(w[...], jnp.concatenate([high, mid], axis=1))
        v[...] = most[:, 0:128] + (most[:, 128:256] + mm(w[...], low))

    def blend(src):
        both = mm(mix[...], split(stacked(src), 3, 0))
        return jnp.where(iota((128, 128), 1) < 64, both[:128], pltpu.roll(both[128:], 64, 1))

    lane_col = iota((1, 1, 128), 2)

    def send_sums(name, u, base, scalars):
        own = pltpu.roll(u, 64, 1).reshape(G, 8, 128)
        now = folded(u)
        u = u.reshape(G, 8, 128)
        c_put[:, base:base + 4] = jnp.where(lane_col < 64, u[:, 0:4], own[:, 4:8])
        if scalars:
            now = u[:, 0:4]
        for i, scalar in enumerate(scalars):
            at = (iota((1, 4, 128), 1) == i) & (iota((1, 4, 128), 2) < 64)
            now = jnp.where(at, jnp.broadcast_to(scalar.reshape(1, 1, 1), (1, 4, 128)), now)
        box(name + "c_out")[0][...] = now
        send(name + "c_out")

    c_put = box("c_put")[0]

    src = arrived("gc_in")
    send_sums("g", blend(src), 0, ())
    rows_b = rows_of(["gb_in"])
    serve(same_b, rows_b, ["gb_out"])
    rows_a = rows_of(names_of("ga_in"))
    serve(same_a, rows_a, names_of("ga_out"))
    fold(wb, rows_b, gb)
    fold(wa, rows_a, ga)
    settle("ga_in0", "gb_in", "gc_in", "a_slices", "b_slices", "c_own", "c_slots", "a_slots0")
    g_part = norm(ga[...] * ga[...] + gb[...] * gb[...])

    def direction_bc(name):
        src = arrived(name + "b_out")
        unpack(src, db, range(T))
        src = arrived(name + "c_out")
        total = jnp.sum(src[...], axis=0)
        turned = turned_of(total if total.shape[0] == 4 else unfolded(total))
        du = columns(turned)
        for t in range(T):
            high, low = split(jnp.transpose(db[t] * depth[t] + tb[t] * du[t]), 2, None)
            left[t, :, 64:128] = high
            left[t, :, 192:256] = high
            left[t, :, 320:384] = low
        return total, turned[64:128]

    def direction_a(name, number, slots):
        src = arrived(name + "a_out" + str(number))
        unpack(src, da, slots)
        products = []
        for t in slots:
            high, low = split(da[t], 2, None)
            right = [high, a3[t, 0:64], low, a3[t, 64:128], high, a3[t, 0:64]]
            products.append(mm(left[t], jnp.concatenate(right, axis=0)) * live(t))
        return products

    _, dirs_g = direction_bc("g")
    g_part = g_part + norm(cols_g[:, 0:8] * dirs_g)

    def second_values(number, slots):
        products = direction_a("g", number, slots)
        for t, product in zip(slots, products):
            jg[t] = product
        return products

    def first_scalars():
        squares = jnp.zeros((128, 128), F32)
        for t in range(T):
            squares = squares + jg[t] * jg[t]
        return g_part, norm(squares)

    cols_w = gradients(second_values, "w", first_scalars)
    settle("ga_out0", "gb_out")

    src = arrived("wc_in")
    group = jnp.sum(src[...], axis=0)
    send_sums("w", blend(src), 4, (group[0:1, 127:128], group[1:2, 127:128]))
    rows_b = rows_of(["wb_in"])
    serve(same_b, rows_b, ["wb_out"])
    rows_a = rows_of(names_of("wa_in"))
    serve(same_a, rows_a, names_of("wa_out"))
    fold(wb, rows_b, vb)
    fold(wa, rows_a, va)
    total_w, dirs_w = direction_bc("w")
    lam = damp[0]
    g_norm = total_w[0:1, 0:1]
    j_norm = total_w[1:2, 0:1]
    alpha0 = g_norm / (j_norm + lam * g_norm)

    def residual_of(g, w):
        return g - alpha0 * (w + lam * g)

    r_a = residual_of(ga[...], va[...])
    r_b = residual_of(gb[...], vb[...])
    r_cols = residual_of(cols_g[:, 0:8], cols_w[:, 0:8])
    rr_part = norm(r_a * r_a + r_b * r_b) + norm(r_cols * residual_of(dirs_g, dirs_w))
    rg_part = norm(r_a * ga[...] + r_b * gb[...]) + norm(r_cols * dirs_g)
    square = jnp.zeros((128, 128), F32)
    cross = jnp.zeros((128, 128), F32)
    for number, slots in enumerate(SLOTS):
        for t, product in zip(slots, direction_a("w", number, slots)):
            jr = residual_of(jg[t], product)
            square = square + jr * jr
            cross = cross + jr * jg[t]

    parts = (rr_part, rg_part, norm(square), norm(cross))
    row = zero_row
    for i, part in enumerate(parts):
        row = jnp.where(lane // 32 == i, part, row)
    out = box("sum_col")[0]
    for j in range(G):
        out[j] = row
    send("sum_col")
    a_put, b_put = box("a_put")[0], box("b_put")[0]
    for j in range(G):
        a_put[j, 0:4] = ga[4 * j:4 * j + 4]
        a_put[j, 4:8] = va[4 * j:4 * j + 4]
        b_put[j, 0:4] = gb[4 * j:4 * j + 4]
        b_put[j, 4:8] = vb[4 * j:4 * j + 4]
    send("a_put")
    send("b_put")
    send("c_put")

    src = arrived("sum_col")
    row = jnp.sum(src[...], axis=0)
    out = box("sum_row")[0]
    for j in range(G):
        out[j] = row
    send("sum_row")
    src_a = arrived("a_put")
    src_b = arrived("b_put")
    own = jnp.sum(arrived("c_put")[...], axis=0)
    own_g = jnp.concatenate([own[0:4, 0:64], own[0:4, 64:128]], axis=0)
    own_w = jnp.concatenate([own[4:8, 0:64], own[4:8, 64:128]], axis=0)
    for j in range(G):
        ga[4 * j:4 * j + 4] = src_a[j, 0:4]
        va[4 * j:4 * j + 4] = src_a[j, 4:8]
        gb[4 * j:4 * j + 4] = src_b[j, 0:4]
        vb[4 * j:4 * j + 4] = src_b[j, 4:8]
    blocks = ((ga[...], va[...], out_a), (gb[...], vb[...], out_b), (own_g, own_w, out_c))
    bases = [(alpha0 * g, residual_of(g, w), g, out) for g, w, out in blocks]
    src = arrived("sum_row")
    row = jnp.sum(src[...], axis=0)
    r_norm, r_g, jr_norm, jr_jg = [row[:, 32 * i:32 * i + 1] for i in range(4)]
    beta = r_norm / g_norm
    curve = (
        jr_norm + lam * r_norm
        + 2.0 * beta * (jr_jg + lam * r_g)
        + beta * beta * (j_norm + lam * g_norm)
    )
    alpha1 = r_norm / curve

    for base, r, g, out in bases:
        out[...] = base + alpha1 * (r + beta * g)
    settle(*list(left_over))


def put(a, b, c, x, y, z):
    x[...] = a[...]
    y[...] = b[...]
    z[...] = c[...]


def per_device(
    tile_data, tile_coords, tile_counts, factor_rows, factor_cols, factor_depth, damping
):
    vmem = pl.BlockSpec(memory_space=pltpu.VMEM)
    boxes = [pltpu.VMEM((G, rows, 128), F32) for _, _, rows in EXCHANGES]
    blocks = ((64, 128), (64, 128), (8, 64))
    steps = pl.pallas_call(
        kernel,
        out_shape=tuple(pltpu.VMEM(block, F32) for block in blocks),
        in_specs=[pl.BlockSpec(memory_space=pltpu.HBM)] * 7,
        out_specs=(vmem, vmem, vmem),
        scratch_shapes=[
            *boxes, *boxes,
            pltpu.SMEM((3, T), jnp.int32), pltpu.SMEM((1,), jnp.int32), pltpu.SMEM((1,), F32),
            pltpu.VMEM((64, 128), F32), pltpu.VMEM((64, 128), F32), pltpu.VMEM((8, 64), F32),
            pltpu.VMEM((T, 128, 128), BF16),
            *[pltpu.VMEM((64, 128), F32)] * 4,
            *[pltpu.VMEM((T, 64, 128), F32)] * 4,
            pltpu.VMEM((T, 128, 128), F32),
            pltpu.VMEM((T, 128, 192), BF16),
            pltpu.VMEM((T, 64, 384), BF16), pltpu.VMEM((T, 64, 384), BF16),
            pltpu.VMEM((T, 192, 128), BF16),
            pltpu.VMEM((T, 128, 384), BF16),
            pltpu.VMEM((T, 128, 128), F32),
            pltpu.VMEM((64, 128), F32),
            pltpu.VMEM((64, 256), BF16), pltpu.VMEM((64, 256), BF16),
            pltpu.VMEM((256, 192), BF16), pltpu.VMEM((256, 192), BF16),
            pltpu.VMEM((256, 256), BF16), pltpu.VMEM((256, 256), BF16),
            pltpu.VMEM((256, 192), BF16),
            pltpu.SemaphoreType.DMA((7,)),
            pltpu.SemaphoreType.DMA((len(FIRST),)),
            pltpu.SemaphoreType.DMA((len(FIRST),)),
        ],
        compiler_params=pltpu.CompilerParams(collective_id=0, has_side_effects=True),
        name="gauss_newton",
    )(
        tile_coords, tile_counts, damping.reshape(1),
        factor_rows, factor_cols, factor_depth.T, tile_data,
    )
    step_a, step_b, step_c = pl.pallas_call(
        put,
        out_shape=tuple(jax.ShapeDtypeStruct(block, F32) for block in blocks),
        in_specs=[vmem, vmem, vmem],
        out_specs=(vmem, vmem, vmem),
        name="put",
    )(*[pltpu.with_memory_space_constraint(step, pltpu.VMEM) for step in steps])
    return step_a, step_b, step_c.T


def solution(mesh):
    both = ("row", "col")
    flip = ("col", "row")
    return jax.shard_map(
        per_device,
        mesh=mesh,
        in_specs=(
            P(both, None, None), P(None, both), P(both),
            P(None, both), P(None, flip), P(None, both), P(),
        ),
        out_specs=(P(None, both), P(None, flip), P(None, both)),
        check_vma=False,
    )
```
